32 devices in a mesh: data: 2 (over x), ffn: 4 (over z), hid: 4 (over y, core).
Axes of the slice: x: 2, y: 2, z: 4, core: 2. Of those that a mesh axis runs over, the one named last changes fastest.
Arguments:
- x_in: bfloat16 [128, 3072], P('data', 'hid'), parts along dimension 0
- gain_one: float32 [3072], P('hid')
- gain_two: float32 [3072], P('hid')
- w_gate: bfloat16 [3072, 24576], P('hid', 'ffn')
- w_up: bfloat16 [3072, 24576], P('hid', 'ffn')
- w_down: bfloat16 [24576, 3072], P('ffn', 'hid')
- w_qkv: bfloat16 [3072, 12288], P('hid', 'ffn')
- dx_out: bfloat16 [128, 3072], P('data', 'hid'), parts along dimension 0
- d_qkv: bfloat16 [128, 12288], P('data', 'ffn'), parts along dimension 0
Outputs:
- output 1: bfloat16 [128, 3072], P('data', 'hid'), parts along dimension 0
- output 2: bfloat16 [6144, 24576], P(('data', 'hid'), 'ffn'), parts along dimension 0
- output 3: bfloat16 [6144, 24576], P(('data', 'hid'), 'ffn'), parts along dimension 0
- output 4: bfloat16 [49152, 3072], P(('data', 'ffn'), 'hid'), parts along dimension 0
- output 5: bfloat16 [6144, 12288], P(('data', 'hid'), 'ffn'), parts along dimension 0
- output 6: float32 [6144], P(('data', 'hid')), parts along dimension 0
- output 7: float32 [6144], P(('data', 'hid')), parts along dimension 0
There are 2 independent parts. The reference program is written for one: setup_inputs(seed, part) draws one part's arguments, and reference() takes and returns one part's arrays. A program takes and returns all parts, laid end to end along the dimension named above; an argument that names none is the same for every part.
All inputs are finite; a program needn't handle non-finite values.
Results may differ from the reference program's by a relative error of at most 0.00629433.
Values are sent between devices in bfloat16 or wider.
A program may use at most 1 GiB of HBM per device.

```python
import jax
import jax.numpy as jnp
from jax import lax

D_MODEL = 3072
D_FF = 24576
Q_HEADS = 16
KV_HEADS = 16
HEAD_DIM = 256
TOKENS = 64
QKV_WIDTH = (Q_HEADS + 2 * KV_HEADS) * HEAD_DIM
NORM_EPS = 1e-6


def norm_forward(z_val, gain_vec):
    inv_rms = lax.rsqrt(jnp.sum(z_val * z_val, axis=-1, keepdims=True) / D_MODEL + NORM_EPS)
    return inv_rms, (z_val * inv_rms * gain_vec).astype(jnp.bfloat16)


def norm_backward(z_val, gain_vec, inv_rms, d_norm):
    g_dn = gain_vec * d_norm
    dot_tok = jnp.sum(g_dn * z_val, axis=-1, keepdims=True)
    d_input = inv_rms * g_dn - z_val * (inv_rms ** 3) * (dot_tok / D_MODEL)
    d_gain = jnp.sum(d_norm * z_val * inv_rms, axis=0)
    return d_input, d_gain


def forward_states(x_in, gain_one, gain_two, w_gate, w_up, w_down):
    x_f32 = x_in.astype(jnp.float32)
    inv_one, normed_one = norm_forward(x_f32, gain_one)
    gate_pre = jnp.dot(normed_one, w_gate, preferred_element_type=jnp.float32)
    up_pre = jnp.dot(normed_one, w_up, preferred_element_type=jnp.float32)
    act_bf = (jax.nn.silu(gate_pre) * up_pre).astype(jnp.bfloat16)
    down_out = jnp.dot(act_bf, w_down, preferred_element_type=jnp.float32)
    resid_f32 = (x_f32 + down_out).astype(jnp.bfloat16).astype(jnp.float32)
    inv_two, normed_two = norm_forward(resid_f32, gain_two)
    return x_f32, inv_one, normed_one, gate_pre, up_pre, act_bf, resid_f32, inv_two, normed_two


def setup_inputs(seed: int = 0, part: int = 0) -> dict:
    shared_keys = jax.random.split(jax.random.key(seed), 6)
    part_keys = jax.random.split(jax.random.fold_in(jax.random.key(seed + 1), part), 6)
    positions = jnp.arange(D_MODEL, dtype=jnp.float32) / D_MODEL
    row_scale = jnp.exp(jax.random.uniform(part_keys[0], (TOKENS, 1), minval=-1.0, maxval=1.0))
    amplitude = jax.random.uniform(part_keys[1], (TOKENS, 1), minval=0.6, maxval=1.2)
    phase_off = jax.random.uniform(part_keys[2], (TOKENS, 1))
    profile = jnp.exp(amplitude * jnp.sin(2.0 * jnp.pi * (positions + phase_off)))
    x_in = (jax.random.normal(part_keys[3], (TOKENS, D_MODEL)) * row_scale * profile).astype(jnp.bfloat16)
    gain_one = jax.random.uniform(shared_keys[0], (D_MODEL,), minval=0.5, maxval=1.5)
    gain_two = jax.random.uniform(shared_keys[1], (D_MODEL,), minval=0.5, maxval=1.5)
    w_gate = (jax.random.normal(shared_keys[2], (D_MODEL, D_FF)) * D_MODEL ** -0.5).astype(jnp.bfloat16)
    w_up = (jax.random.normal(shared_keys[3], (D_MODEL, D_FF)) * D_MODEL ** -0.5).astype(jnp.bfloat16)
    w_down = (jax.random.normal(shared_keys[4], (D_FF, D_MODEL)) * D_FF ** -0.5).astype(jnp.bfloat16)
    w_qkv = (jax.random.normal(shared_keys[5], (D_MODEL, QKV_WIDTH)) * D_MODEL ** -0.5).astype(jnp.bfloat16)
    states = forward_states(x_in, gain_one, gain_two, w_gate, w_up, w_down)
    qkv_est = jnp.dot(states[8], w_qkv, preferred_element_type=jnp.float32)
    d_qkv = (qkv_est + 0.5 * jax.random.normal(part_keys[4], (TOKENS, QKV_WIDTH))).astype(jnp.bfloat16)
    dx_out = (3.0 * (states[6] - states[0]) + 0.5 * jax.random.normal(part_keys[5], (TOKENS, D_MODEL))).astype(jnp.bfloat16)
    return {"x_in": x_in, "gain_one": gain_one, "gain_two": gain_two, "w_gate": w_gate, "w_up": w_up, "w_down": w_down, "w_qkv": w_qkv, "dx_out": dx_out, "d_qkv": d_qkv}


def reference(x_in, gain_one, gain_two, w_gate, w_up, w_down, w_qkv, dx_out, d_qkv):
    x_f32, inv_one, normed_one, gate_pre, up_pre, act_bf, resid_f32, inv_two, normed_two = forward_states(x_in, gain_one, gain_two, w_gate, w_up, w_down)
    dw_qkv = jnp.dot(normed_two.T, d_qkv, preferred_element_type=jnp.float32).astype(jnp.bfloat16)
    d_normed_two = jnp.dot(d_qkv, w_qkv.T, preferred_element_type=jnp.float32)
    d_resid, d_gain_two = norm_backward(resid_f32, gain_two, inv_two, d_normed_two)
    d_res_tot = dx_out.astype(jnp.float32) + d_resid
    d_res_bf = d_res_tot.astype(jnp.bfloat16)
    dw_down = jnp.dot(act_bf.T, d_res_bf, preferred_element_type=jnp.float32).astype(jnp.bfloat16)
    d_act = jnp.dot(d_res_bf, w_down.T, preferred_element_type=jnp.float32)
    gate_sig = jax.nn.sigmoid(gate_pre)
    d_gate = (d_act * up_pre * gate_sig * (1.0 + gate_pre * (1.0 - gate_sig))).astype(jnp.bfloat16)
    d_up = (d_act * jax.nn.silu(gate_pre)).astype(jnp.bfloat16)
    dw_gate = jnp.dot(normed_one.T, d_gate, preferred_element_type=jnp.float32).astype(jnp.bfloat16)
    dw_up = jnp.dot(normed_one.T, d_up, preferred_element_type=jnp.float32).astype(jnp.bfloat16)
    d_normed_one = jnp.dot(d_gate, w_gate.T, preferred_element_type=jnp.float32) + jnp.dot(d_up, w_up.T, preferred_element_type=jnp.float32)
    d_in, d_gain_one = norm_backward(x_f32, gain_one, inv_one, d_normed_one)
    dx_in = (d_res_tot + d_in).astype(jnp.bfloat16)
    return (dx_in, dw_gate, dw_up, dw_down, dw_qkv, d_gain_one, d_gain_two)
```

```python
import functools
import jax
import jax.numpy as jnp
from jax import lax
from jax.experimental import pallas as pl
from jax.experimental.pallas import tpu as pltpu
from jax.sharding import PartitionSpec as P

NORM_EPS = 1e-6
MESH = pl.DeviceIdType.MESH
ANY = pl.BlockSpec(memory_space=pl.ANY)
VM = pl.BlockSpec(memory_space=pltpu.VMEM)
BF = jnp.bfloat16
F32 = jnp.float32
LANES = 128


def dot_nn(a_mat, b_mat):
    return lax.dot_general(a_mat, b_mat, (((1,), (0,)), ((), ())), preferred_element_type=F32)


def dot_nt(a_mat, b_mat):
    return lax.dot_general(a_mat, b_mat, (((1,), (1,)), ((), ())), preferred_element_type=F32)


def dot_tn(a_mat, b_mat):
    return lax.dot_general(a_mat, b_mat, (((0,), (0,)), ((), ())), preferred_element_type=F32)


def step_kernel(
    dims,
    x_h, g1_ref, g2_ref, wg_h, wu_h, wd_h, wq_h, dxo_h, dq_h,
    dx_o, dg1_o, dg2_o, n1_o, dgu_o, dwq_o, dwd_o,
    xv, dxv, dqv, wqv, wgv, wuv, wdv,
    n1v, n2v, ebv, ev, acc, own1, d2s, d2r, ys, yr, gu, av,
    own2, e2s, e2r, ys2, yr2, dgu,
    dn2r, zs, zr, x2v, zs2, zr2, dn1v, st1, st2, st3, dxr,
    ld_sem, w_sem, out_sem,
    d2_ss, d2_rs, y_ss, y_rs, ag_ss, ag_rs, z_ss, z_rs, st_ss, st_rs,
):
    n_chunk, n_ffn, d_model = dims
    tokens, width = xv.shape
    rows = tokens // 4
    ffn_w = wgv.shape[1]
    cw = ffn_w // n_chunk
    tile = min(512, cw)

    hid = lax.axis_index("hid")
    ffn = lax.axis_index("ffn")
    chip, core = hid // 2, hid % 2
    core_peer = 2 * chip + (1 - core)
    chip_peer = 2 * (1 - chip) + core
    diag_peer = 2 * (1 - chip) + (1 - core)

    def true_row(block):
        return rows * (2 * ((block // 2 + core) % 2) + (block % 2 + chip) % 2)

    def rcopy(src, dst, ss, rs, dev):
        return pltpu.make_async_remote_copy(
            src_ref=src, dst_ref=dst, send_sem=ss, recv_sem=rs, device_id=dev, device_id_type=MESH)

    def load_rows(src, dst, slot):
        cps = []
        for j in range(4):
            r = pl.multiple_of(true_row(j), rows)
            cps.append(pltpu.make_async_copy(
                src.at[pl.ds(r, rows), :], dst.at[pl.ds(rows * j, rows), :], ld_sem.at[slot + j]))
        return cps

    def w_load(i):
        cols = pl.ds(i * cw, cw)
        return [
            pltpu.make_async_copy(wg_h.at[:, cols], wgv.at[:, cols], w_sem.at[0, i]),
            pltpu.make_async_copy(wu_h.at[:, cols], wuv.at[:, cols], w_sem.at[1, i]),
        ]

    def wd_load(i):
        cols = pl.ds(i * cw, cw)
        return pltpu.make_async_copy(wd_h.at[cols, :], wdv.at[cols, :], w_sem.at[2, i])

    x_cp = load_rows(x_h, xv, 0)
    dq_cp = load_rows(dq_h, dqv, 4)
    dx_cp = load_rows(dxo_h, dxv, 8)
    wq_cp = pltpu.make_async_copy(wq_h, wqv, ld_sem.at[12])
    for c in x_cp:
        c.start()
    for c in dq_cp:
        c.start()
    wq_cp.start()
    w_cps = [w_load(i) for i in range(n_chunk)]
    wd_cps = [wd_load(i) for i in range(n_chunk)]
    for i in range(min(2, n_chunk)):
        for c in w_cps[i]:
            c.start()

    barrier = pltpu.get_barrier_semaphore()
    peers = []
    for dh in range(4):
        for df in range(n_ffn):
            if dh or df:
                peers.append({"hid": (hid + dh) % 4, "ffn": (ffn + df) % n_ffn})
    for dev in peers:
        pl.semaphore_signal(barrier, inc=1, device_id=dev, device_id_type=MESH)

    lane = lax.broadcasted_iota(jnp.int32, (tokens, LANES), 1)
    row = lax.broadcasted_iota(jnp.int32, (tokens, LANES), 0)
    tok_id = rows * (2 * ((row // (2 * rows) + core) % 2) + ((row // rows) % 2 + chip) % 2) + row % rows

    for c in x_cp:
        c.wait()
    xf = xv[...].astype(F32)
    ssq = jnp.sum(xf * xf, axis=1, keepdims=True)
    st1[hid] = jnp.sum(jnp.where(lane == tok_id, ssq, 0.0), axis=0, keepdims=True)
    pl.semaphore_wait(barrier, len(peers))
    st1_cps = []
    for k, dev in enumerate((core_peer, chip_peer, diag_peer)):
        c = rcopy(st1.at[hid], st1.at[hid], st_ss.at[0, k], st_rs.at[0, hid], {"hid": dev})
        c.start()
        st1_cps.append(c)

    for c in dq_cp:
        c.wait()
    wq_cp.wait()
    for i in range(n_chunk):
        if i >= 2:
            for c in w_cps[i]:
                c.start()
    for i in range(n_chunk):
        wd_cps[i].start()
    for c in dx_cp:
        c.start()
    qk = min(768, dqv.shape[1])
    acc[...] = dot_nt(dqv[:, :qk], wqv[:, :qk])

    def dn2_body(k, _):
        cols = pl.ds(pl.multiple_of(k * qk, qk), qk)
        acc[...] += dot_nt(dqv[:, cols], wqv[:, cols])
        return 0
    lax.fori_loop(1, dqv.shape[1] // qk, dn2_body, 0)
    dn2r[ffn] = acc[...].astype(BF)
    dn2_cps = []
    for df in range(1, n_ffn):
        c = rcopy(dn2r.at[ffn], dn2r.at[ffn], z_ss.at[0, df], z_rs.at[0, ffn], {"ffn": (ffn + df) % n_ffn})
        c.start()
        dn2_cps.append(c)

    for dev in (core_peer, chip_peer, diag_peer):
        rcopy(st1.at[dev], st1.at[dev], st_ss.at[0, 0], st_rs.at[0, dev], {"hid": dev}).wait_recv()
    tot1 = (st1[0] + st1[1]) + (st1[2] + st1[3])
    mean1 = jnp.sum(jnp.where(lane == tok_id, tot1, 0.0), axis=1, keepdims=True) / d_model
    inv1 = lax.rsqrt(mean1 + NORM_EPS)
    g1v = g1_ref[...]
    g2v = g2_ref[...]
    n1v[...] = (xf * inv1 * g1v).astype(BF)
    n1_cp = pltpu.make_async_copy(n1v, n1_o, out_sem.at[n_chunk])
    n1_cp.start()

    half = 2 * rows
    sends = []

    def fwd_a(i):
        for c in w_cps[i]:
            c.wait()
        for w_ref, base in ((wgv, 0), (wuv, cw)):
            def body(t, _, w_ref=w_ref, base=base):
                p = dot_nn(n1v[...], w_ref[:, pl.ds(pl.multiple_of(i * cw + t * tile, tile), tile)])
                dst = pl.ds(pl.multiple_of(base + t * tile, tile), tile)
                own1[i, :, dst] = p[:half]
                d2s[i, :, dst] = p[half:].astype(BF)
                return 0
            lax.fori_loop(0, cw // tile, body, 0)
        c = rcopy(d2s.at[i], d2r.at[i], d2_ss.at[0, i], d2_rs.at[0, i], {"hid": core_peer})
        c.start()
        sends.append(c)

    def fwd_b(i):
        rcopy(d2s.at[i], d2r.at[i], d2_ss.at[0, i], d2_rs.at[0, i], {"hid": core_peer}).wait_recv()
        ys[i] = (own1[i, rows:half] + d2r[i, rows:half].astype(F32)).astype(BF)
        c = rcopy(ys.at[i], yr.at[i], y_ss.at[0, i], y_rs.at[0, i], {"hid": chip_peer})
        c.start()
        sends.append(c)
        gu[i] = own1[i, :rows] + d2r[i, :rows].astype(F32)

    def fwd_c(i):
        rcopy(ys.at[i], yr.at[i], y_ss.at[0, i], y_rs.at[0, i], {"hid": chip_peer}).wait_recv()
        tot = gu[i] + yr[i].astype(F32)
        gu[i] = tot
        g, u = tot[:, :cw], tot[:, cw:]
        av[i, :rows] = (jax.nn.silu(g) * u).astype(BF)
        own = av.at[i, pl.ds(0, rows)]
        c = rcopy(own, av.at[i, pl.ds(rows, rows)], ag_ss.at[0, 0, i], ag_rs.at[0, 0, i], {"hid": chip_peer})
        c.start()
        sends.append(c)
        c = rcopy(own, av.at[i, pl.ds(2 * rows, rows)], ag_ss.at[0, 1, i], ag_rs.at[0, 1, i], {"hid": core_peer})
        c.start()
        sends.append(c)

    def ag_wait(buf, ph, lvl, i):
        blk = buf.at[i, pl.ds((lvl + 1) * rows, rows)]
        rcopy(blk, blk, ag_ss.at[ph, lvl, i], ag_rs.at[ph, lvl, i], {"hid": core_peer}).wait_recv()

    def ag_forward(buf, ph, i):
        ag_wait(buf, ph, 0, i)
        c = rcopy(buf.at[i, pl.ds(rows, rows)], buf.at[i, pl.ds(3 * rows, rows)],
                  ag_ss.at[ph, 2, i], ag_rs.at[ph, 2, i], {"hid": core_peer})
        c.start()
        sends.append(c)

    def fwd_e(i):
        ag_wait(av, 0, 1, i)
        ag_wait(av, 0, 2, i)
        wd_cps[i].wait()
        p = dot_nn(av[i], wdv[i * cw:(i + 1) * cw, :])
        if i == 0:
            acc[...] = p
        else:
            acc[...] += p

    def pipeline(stages):
        last = max(lag for _, lag in stages)
        for s in range(n_chunk + last):
            for fn, lag in stages:
                if 0 <= s - lag < n_chunk:
                    fn(s - lag)

    pipeline([(fwd_a, 0), (fwd_b, 1), (fwd_c, 4), (lambda i: ag_forward(av, 0, i), 6), (fwd_e, 7)])

    def z_scatter(sb, rb, ph):
        sb[...] = acc[...].astype(BF)
        for df in range(1, n_ffn):
            to = (ffn + df) % n_ffn
            c = rcopy(sb.at[pl.ds(pl.multiple_of(rows * to, rows), rows)], rb.at[df - 1],
                      z_ss.at[ph, df], z_rs.at[ph, df], {"ffn": to})
            c.start()
            sends.append(c)

    def z_total(sb, rb, ph):
        tot = acc[pl.ds(pl.multiple_of(rows * ffn, rows), rows), :]
        for df in range(1, n_ffn):
            rcopy(rb.at[df - 1], rb.at[df - 1], z_ss.at[ph, df], z_rs.at[ph, df], {"ffn": ffn}).wait_recv()
            tot = tot + rb[df - 1].astype(F32)
        return tot

    def z_gather(buf, ph):
        mine = buf.at[pl.ds(pl.multiple_of(rows * ffn, rows), rows)]
        for df in range(1, n_ffn):
            c = rcopy(mine, mine, z_ss.at[ph, df], z_rs.at[ph, ffn], {"ffn": (ffn + df) % n_ffn})
            c.start()
            sends.append(c)

    def z_gather_wait(buf, ph):
        for df in range(1, n_ffn):
            frm = (ffn + df) % n_ffn
            blk = buf.at[pl.ds(pl.multiple_of(rows * frm, rows), rows)]
            rcopy(blk, blk, z_ss.at[ph, df], z_rs.at[ph, frm], {"ffn": frm}).wait_recv()

    def stat_send(st, k, ssq_v, c_v):
        ln = lax.broadcasted_iota(jnp.int32, (rows, LANES), 1)
        rw = lax.broadcasted_iota(jnp.int32, (rows, LANES), 0)
        tid = true_row(ffn) + rw
        val = jnp.where(ln == tid + tokens, c_v, 0.0)
        if ssq_v is not None:
            val = val + jnp.where(ln == tid, ssq_v, 0.0)
        me = hid * n_ffn + ffn
        st[me] = jnp.sum(val, axis=0, keepdims=True)
        for j, dev in enumerate(peers):
            c = rcopy(st.at[me], st.at[me], st_ss.at[k, j], st_rs.at[k, me], dev)
            c.start()
            sends.append(c)

    def stat_total(st, k):
        for j, dev in enumerate(peers):
            slot = dev["hid"] * n_ffn + dev["ffn"]
            rcopy(st.at[slot], st.at[slot], st_ss.at[k, j], st_rs.at[k, slot], dev).wait_recv()
        tot = st[0]
        for s in range(1, 4 * n_ffn):
            tot = tot + st[s]
        return tot

    z_scatter(zs, zr, 1)
    for df in range(1, n_ffn):
        frm = (ffn + df) % n_ffn
        rcopy(dn2r.at[frm], dn2r.at[frm], z_ss.at[0, df], z_rs.at[0, frm], {"ffn": frm}).wait_recv()
    dn2_tot = dn2r[0].astype(F32)
    for s in range(1, n_ffn):
        dn2_tot = dn2_tot + dn2r[s].astype(F32)
    ev[...] = dn2_tot
    my_rows = pl.ds(pl.multiple_of(rows * ffn, rows), rows)
    x2_rows = (xv[my_rows, :].astype(F32) + z_total(zs, zr, 1)).astype(BF)
    x2v[my_rows, :] = x2_rows
    z_gather(x2v, 2)
    x2_f = x2_rows.astype(F32)
    stat_send(st2, 1,
              jnp.sum(x2_f * x2_f, axis=1, keepdims=True),
              jnp.sum(g2v * x2_f * ev[my_rows, :], axis=1, keepdims=True))
    for c in dx_cp:
        c.wait()
    z_gather_wait(x2v, 2)
    tot2 = stat_total(st2, 1)
    inv2 = lax.rsqrt(jnp.sum(jnp.where(lane == tok_id, tot2, 0.0), axis=1, keepdims=True) / d_model + NORM_EPS)
    c2 = jnp.sum(jnp.where(lane == tok_id + tokens, tot2, 0.0), axis=1, keepdims=True)
    x2f = x2v[...].astype(F32)
    dn2 = ev[...]
    n2v[...] = (x2f * inv2 * g2v).astype(BF)
    e_val = dxv[...].astype(F32) + (inv2 * (g2v * dn2) - x2f * (inv2 ** 3) * (c2 / d_model))
    dg2_o[...] = jnp.sum(dn2 * x2f * inv2, axis=0, keepdims=True)
    ev[...] = e_val
    ebv[...] = e_val.astype(BF)

    def bwd_a(i):
        def body(t, _):
            p = dot_nt(ebv[...], wdv[pl.ds(pl.multiple_of(i * cw + t * tile, tile), tile), :])
            dst = pl.ds(pl.multiple_of(t * tile, tile), tile)
            own2[i, :, dst] = p[:half]
            e2s[i, :, dst] = p[half:].astype(BF)
            return 0
        lax.fori_loop(0, cw // tile, body, 0)
        c = rcopy(e2s.at[i], e2r.at[i], d2_ss.at[1, i], d2_rs.at[1, i], {"hid": core_peer})
        c.start()
        sends.append(c)

    def bwd_b(i):
        rcopy(e2s.at[i], e2r.at[i], d2_ss.at[1, i], d2_rs.at[1, i], {"hid": core_peer}).wait_recv()
        ys2[i] = (own2[i, rows:half] + e2r[i, rows:half].astype(F32)).astype(BF)
        c = rcopy(ys2.at[i], yr2.at[i], y_ss.at[1, i], y_rs.at[1, i], {"hid": chip_peer})
        c.start()
        sends.append(c)

    def bwd_c(i):
        rcopy(ys2.at[i], yr2.at[i], y_ss.at[1, i], y_rs.at[1, i], {"hid": chip_peer}).wait_recv()
        d_act = own2[i, :rows] + e2r[i, :rows].astype(F32) + yr2[i].astype(F32)
        g, u = gu[i, :, :cw], gu[i, :, cw:]
        sig = jax.nn.sigmoid(g)
        dgu[i, :rows, :cw] = (d_act * u * sig * (1.0 + g * (1.0 - sig))).astype(BF)
        dgu[i, :rows, cw:] = (d_act * (g * sig)).astype(BF)
        own = dgu.at[i, pl.ds(0, rows)]
        c = rcopy(own, dgu.at[i, pl.ds(rows, rows)], ag_ss.at[1, 0, i], ag_rs.at[1, 0, i], {"hid": chip_peer})
        c.start()
        sends.append(c)
        c = rcopy(own, dgu.at[i, pl.ds(2 * rows, rows)], ag_ss.at[1, 1, i], ag_rs.at[1, 1, i], {"hid": core_peer})
        c.start()
        sends.append(c)

    out_cps = []

    def bwd_e(i):
        ag_wait(dgu, 1, 1, i)
        ag_wait(dgu, 1, 2, i)
        c = pltpu.make_async_copy(dgu.at[i], dgu_o.at[i], out_sem.at[i])
        c.start()
        out_cps.append(c)
        cols = pl.ds(i * cw, cw)
        p = dot_nt(dgu[i, :, :cw], wgv[:, cols]) + dot_nt(dgu[i, :, cw:], wuv[:, cols])
        if i == 0:
            acc[...] = p
        else:
            acc[...] += p

    piece = min(256, cw)

    def fill_down(i):
        for t in range(cw // piece):
            r = i * cw + t * piece
            dwd_o[r:r + piece, :] = dot_tn(av[i, :, t * piece:(t + 1) * piece], ebv[...]).astype(BF)

    pipeline([(bwd_a, 0), (fill_down, 0), (bwd_b, 1), (bwd_c, 3), (lambda i: ag_forward(dgu, 1, i), 5), (bwd_e, 6)])

    z_scatter(zs2, zr2, 3)
    qt = min(512, dqv.shape[1])

    def fill_qkv(k, _):
        cols = pl.ds(pl.multiple_of(k * qt, qt), qt)
        dwq_o[:, cols] = dot_tn(n2v[...], dqv[:, cols]).astype(BF)
        return 0
    lax.fori_loop(0, dqv.shape[1] // qt, fill_qkv, 0)
    dn1_rows = z_total(zs2, zr2, 3).astype(BF)
    dn1v[my_rows, :] = dn1_rows
    z_gather(dn1v, 4)
    stat_send(st3, 2, None,
              jnp.sum(g1v * xv[my_rows, :].astype(F32) * dn1_rows.astype(F32), axis=1, keepdims=True))
    z_gather_wait(dn1v, 4)
    tot3 = stat_total(st3, 2)
    c1 = jnp.sum(jnp.where(lane == tok_id + tokens, tot3, 0.0), axis=1, keepdims=True)
    xf = xv[...].astype(F32)
    dn1 = dn1v[...].astype(F32)
    dxr[...] = (ev[...] + (inv1 * (g1v * dn1) - xf * (inv1 ** 3) * (c1 / d_model))).astype(BF)
    dg1_o[...] = jnp.sum(dn1 * xf * inv1, axis=0, keepdims=True)
    for j in range(4):
        r = pl.multiple_of(true_row(j), rows)
        c = pltpu.make_async_copy(dxr.at[pl.ds(rows * j, rows), :], dx_o.at[pl.ds(r, rows), :], ld_sem.at[j])
        c.start()
        out_cps.append(c)
    for c in st1_cps + dn2_cps + sends:
        c.wait_send()
    for c in out_cps:
        c.wait()
    n1_cp.wait()


def grads_kernel(n1_ref, dg_ref, du_ref, dwq_ref, dwd_ref, wg_o, wu_o, wq_o, wd_o, n1t, sem):
    step = pl.program_id(0)
    cps = (pltpu.make_async_copy(dwd_ref, wd_o, sem.at[0]), pltpu.make_async_copy(dwq_ref, wq_o, sem.at[1]))

    @pl.when(step == 0)
    def _():
        for c in cps:
            c.start()
        n1t[...] = jnp.transpose(n1_ref[...])
    wg_o[...] = dot_nn(n1t[...], dg_ref[0]).astype(BF)
    wu_o[...] = dot_nn(n1t[...], du_ref[0]).astype(BF)

    @pl.when(step == pl.num_programs(0) - 1)
    def _():
        for c in cps:
            c.wait()


def solution(mesh):
    n_hid, n_ffn = mesh.shape["hid"], mesh.shape["ffn"]

    def local_step(x_in, gain_one, gain_two, w_gate, w_up, w_down, w_qkv, dx_out, d_qkv):
        tokens, width = x_in.shape
        ffn_w, qkv_w = w_gate.shape[1], w_qkv.shape[1]
        n_chunk = 6
        cw = ffn_w // n_chunk
        rows = tokens // 4
        sds = jax.ShapeDtypeStruct
        vm = pltpu.VMEM
        dma = pltpu.SemaphoreType.DMA
        outs = pl.pallas_call(
            functools.partial(step_kernel, (n_chunk, n_ffn, width * n_hid)),
            out_shape=(
                sds((tokens, width), BF), sds((1, width), F32), sds((1, width), F32),
                sds((tokens, width), BF), sds((n_chunk, tokens, 2 * cw), BF),
                vm((width, qkv_w), BF), vm((ffn_w, width), BF),
            ),
            in_specs=[ANY, VM, VM] + [ANY] * 6,
            out_specs=(ANY, VM, VM, ANY, ANY, VM, VM),
            scratch_shapes=[
                vm((tokens, width), BF), vm((tokens, width), BF), vm((tokens, qkv_w), BF),
                vm((width, qkv_w), BF), vm((width, ffn_w), BF), vm((width, ffn_w), BF), vm((ffn_w, width), BF),
                vm((tokens, width), BF), vm((tokens, width), BF), vm((tokens, width), BF), vm((tokens, width), F32),
                vm((tokens, width), F32),
                vm((n_chunk, 2 * rows, 2 * cw), F32), vm((n_chunk, 2 * rows, 2 * cw), BF), vm((n_chunk, 2 * rows, 2 * cw), BF),
                vm((n_chunk, rows, 2 * cw), BF), vm((n_chunk, rows, 2 * cw), BF), vm((n_chunk, rows, 2 * cw), F32),
                vm((n_chunk, tokens, cw), BF),
                vm((n_chunk, 2 * rows, cw), F32), vm((n_chunk, 2 * rows, cw), BF), vm((n_chunk, 2 * rows, cw), BF),
                vm((n_chunk, rows, cw), BF), vm((n_chunk, rows, cw), BF), vm((n_chunk, tokens, 2 * cw), BF),
                vm((n_ffn, tokens, width), BF),
                vm((tokens, width), BF), vm((n_ffn - 1, rows, width), BF), vm((tokens, width), BF),
                vm((tokens, width), BF), vm((n_ffn - 1, rows, width), BF), vm((tokens, width), BF),
                vm((4, 1, LANES), F32), vm((4 * n_ffn, 1, LANES), F32), vm((4 * n_ffn, 1, LANES), F32),
                vm((tokens, width), BF),
                dma((13,)), dma((3, n_chunk)), dma((n_chunk + 1,)),
                dma((2, n_chunk)), dma((2, n_chunk)), dma((2, n_chunk)), dma((2, n_chunk)),
                dma((2, 3, n_chunk)), dma((2, 3, n_chunk)), dma((5, n_ffn)), dma((5, n_ffn)),
                dma((3, 4 * n_ffn)), dma((3, 4 * n_ffn)),
            ],
            compiler_params=pltpu.CompilerParams(
                collective_id=0, has_side_effects=True, vmem_limit_bytes=48 * 2 ** 20),
            name="block_step",
        )(x_in, gain_one.reshape(1, width), gain_two.reshape(1, width), w_gate, w_up, w_down, w_qkv, dx_out, d_qkv)
        dx_in, dg1, dg2, n1, dgu, dwq_v, dwd_v = outs
        per = max(1, cw // 512)
        tile = cw // per
        dwq_v = pltpu.with_memory_space_constraint(dwq_v, pltpu.VMEM)
        dwd_v = pltpu.with_memory_space_constraint(dwd_v, pltpu.VMEM)
        dw_gate, dw_up, dw_qkv, dw_down = pl.pallas_call(
            grads_kernel,
            grid=(n_chunk * per,),
            out_shape=(sds((width, ffn_w), BF), sds((width, ffn_w), BF), sds((width, qkv_w), BF), sds((ffn_w, width), BF)),
            in_specs=[
                pl.BlockSpec((tokens, width), lambda s: (0, 0)),
                pl.BlockSpec((1, tokens, tile), lambda s: (s // per, 0, s % per)),
                pl.BlockSpec((1, tokens, tile), lambda s: (s // per, 0, per + s % per)),
                VM, VM,
            ],
            out_specs=(
                pl.BlockSpec((width, tile), lambda s: (0, s)), pl.BlockSpec((width, tile), lambda s: (0, s)), ANY, ANY),
            scratch_shapes=[vm((width, tokens), BF), dma((2,))],
            compiler_params=pltpu.CompilerParams(vmem_limit_bytes=24 * 2 ** 20),
            name="weight_grads",
        )(n1, dgu, dgu, dwq_v, dwd_v)
        return dx_in, dw_gate, dw_up, dw_down, dw_qkv, dg1.reshape(width), dg2.reshape(width)

    tok_spec = P("data", "hid")
    in_specs = (tok_spec, P("hid"), P("hid"), P("hid", "ffn"), P("hid", "ffn"), P("ffn", "hid"), P("hid", "ffn"), tok_spec, P("data", "ffn"))
    out_specs = (tok_spec, P(("data", "hid"), "ffn"), P(("data", "hid"), "ffn"), P(("data", "ffn"), "hid"), P(("data", "hid"), "ffn"), P(("data", "hid")), P(("data", "hid")))
    return jax.shard_map(local_step, mesh=mesh, in_specs=in_specs, out_specs=out_specs, check_vma=False)
```

```python
import functools
import jax
import jax.numpy as jnp
from jax import lax
from jax.experimental import pallas as pl
from jax.experimental.pallas import tpu as pltpu
from jax.sharding import PartitionSpec as P

NORM_EPS = 1e-6
MESH = pl.DeviceIdType.MESH
ANY = pl.BlockSpec(memory_space=pl.ANY)
VM = pl.BlockSpec(memory_space=pltpu.VMEM)
BF = jnp.bfloat16
F32 = jnp.float32
LANES = 128
N_CHUNK = 12


def dot_nn(a_mat, b_mat):
    return lax.dot_general(a_mat, b_mat, (((1,), (0,)), ((), ())), preferred_element_type=F32)


def dot_nt(a_mat, b_mat):
    return lax.dot_general(a_mat, b_mat, (((1,), (1,)), ((), ())), preferred_element_type=F32)


def dot_tn(a_mat, b_mat):
    return lax.dot_general(a_mat, b_mat, (((0,), (0,)), ((), ())), preferred_element_type=F32)


class Place:
    def __init__(self, tokens, n_ffn):
        self.tokens, self.rows, self.n_ffn = tokens, tokens // 4, n_ffn
        self.hid = lax.axis_index("hid")
        self.ffn = lax.axis_index("ffn")
        self.chip, self.core = self.hid // 2, self.hid % 2
        self.core_peer = 2 * self.chip + (1 - self.core)
        self.chip_peer = 2 * (1 - self.chip) + self.core
        self.diag_peer = 2 * (1 - self.chip) + (1 - self.core)
        self.peers = []
        for dh in range(4):
            for df in range(n_ffn):
                if dh or df:
                    self.peers.append({"hid": (self.hid + dh) % 4, "ffn": (self.ffn + df) % n_ffn})

    def true_row(self, block):
        return self.rows * (2 * ((block // 2 + self.core) % 2) + (block % 2 + self.chip) % 2)

    def my_rows(self, ffn=None):
        return pl.ds(pl.multiple_of(self.rows * (self.ffn if ffn is None else ffn), self.rows), self.rows)

    def lanes(self):
        lane = lax.broadcasted_iota(jnp.int32, (self.tokens, LANES), 1)
        row = lax.broadcasted_iota(jnp.int32, (self.tokens, LANES), 0)
        rows = self.rows
        tok = rows * (2 * ((row // (2 * rows) + self.core) % 2) + ((row // rows) % 2 + self.chip) % 2) + row % rows
        return lane, tok

    def signal_all(self, barrier):
        for dev in self.peers:
            pl.semaphore_signal(barrier, inc=1, device_id=dev, device_id_type=MESH)


def rcopy(src, dst, ss, rs, dev):
    return pltpu.make_async_remote_copy(
        src_ref=src, dst_ref=dst, send_sem=ss, recv_sem=rs, device_id=dev, device_id_type=MESH)


def z_scatter(pos, part, sb, rb, ss, rs, sends):
    sb[...] = part[...].astype(BF)
    for df in range(1, pos.n_ffn):
        to = (pos.ffn + df) % pos.n_ffn
        c = rcopy(sb.at[pos.my_rows(to)], rb.at[df - 1], ss.at[df], rs.at[df], {"ffn": to})
        c.start()
        sends.append(c)


def z_total(pos, part, rb, ss, rs):
    tot = part[pos.my_rows(), :]
    for df in range(1, pos.n_ffn):
        rcopy(rb.at[df - 1], rb.at[df - 1], ss.at[df], rs.at[df], {"ffn": pos.ffn}).wait_recv()
        tot = tot + rb[df - 1].astype(F32)
    return tot


def z_gather(pos, buf, ss, rs, sends):
    mine = buf.at[pos.my_rows()]
    for df in range(1, pos.n_ffn):
        c = rcopy(mine, mine, ss.at[df], rs.at[pos.ffn], {"ffn": (pos.ffn + df) % pos.n_ffn})
        c.start()
        sends.append(c)


def z_gather_wait(pos, buf, ss, rs):
    for df in range(1, pos.n_ffn):
        frm = (pos.ffn + df) % pos.n_ffn
        blk = buf.at[pos.my_rows(frm)]
        rcopy(blk, blk, ss.at[df], rs.at[frm], {"ffn": frm}).wait_recv()


def stat_send(pos, st, ss, rs, ssq_v, c_v, sends):
    ln = lax.broadcasted_iota(jnp.int32, (pos.rows, LANES), 1)
    tid = pos.true_row(pos.ffn) + lax.broadcasted_iota(jnp.int32, (pos.rows, LANES), 0)
    val = jnp.where(ln == tid + pos.tokens, c_v, 0.0)
    if ssq_v is not None:
        val = val + jnp.where(ln == tid, ssq_v, 0.0)
    me = pos.hid * pos.n_ffn + pos.ffn
    st[me] = jnp.sum(val, axis=0, keepdims=True)
    for j, dev in enumerate(pos.peers):
        c = rcopy(st.at[me], st.at[me], ss.at[j], rs.at[me], dev)
        c.start()
        sends.append(c)


def stat_total(pos, st, ss, rs):
    for j, dev in enumerate(pos.peers):
        slot = dev["hid"] * pos.n_ffn + dev["ffn"]
        rcopy(st.at[slot], st.at[slot], ss.at[j], rs.at[slot], dev).wait_recv()
    tot = st[0]
    for s in range(1, 4 * pos.n_ffn):
        tot = tot + st[s]
    return tot


def step_kernel(
    dims,
    x_h, g1_ref, g2_ref, wg_h, wu_h, wd_h, wq_h, dxo_h, dq_h,
    wg, wu, wd, wq, dx_o, dg1_o, dg2_o,
    xv, ev, dxv, dqv, n1v, n1t, n2v, n2t, ebv, acc, own1, d2s, d2r, ys, yr, gu, av,
    own2, e2s, e2r, ys2, yr2, dgu,
    dn2r, zs, zr, x2v, zs2, zr2, dn1v, st1, st2, st3,
    ld_sem, w_sem,
    d2_ss, d2_rs, y_ss, y_rs, ag_ss, ag_rs, z_ss, z_rs, st_ss, st_rs,
):
    n_chunk, n_ffn, d_model = dims
    tokens, width = xv.shape
    rows = tokens // 4
    half = 2 * rows
    ffn_w = wg.shape[1]
    cw = ffn_w // n_chunk
    pos = Place(tokens, n_ffn)
    barrier = pltpu.get_barrier_semaphore()
    pos.signal_all(barrier)

    def load_rows(src, dst, slot):
        cps = []
        for j in range(4):
            r = pl.multiple_of(pos.true_row(j), rows)
            cps.append(pltpu.make_async_copy(
                src.at[pl.ds(r, rows), :], dst.at[pl.ds(rows * j, rows), :], ld_sem.at[slot + j]))
        return cps

    x_cp = load_rows(x_h, xv, 0)
    dq_cp = load_rows(dq_h, dqv, 4)
    dx_cp = load_rows(dxo_h, dxv, 8)
    wq_cp = pltpu.make_async_copy(wq_h, wq, ld_sem.at[12])
    for c in x_cp:
        c.start()
    for c in dq_cp:
        c.start()
    wq_cp.start()
    w_cps, wd_cps = [], []
    for i in range(n_chunk):
        cols = pl.ds(i * cw, cw)
        w_cps.append([
            pltpu.make_async_copy(wg_h.at[:, cols], wg.at[:, cols], w_sem.at[0, i]),
            pltpu.make_async_copy(wu_h.at[:, cols], wu.at[:, cols], w_sem.at[1, i]),
        ])
        wd_cps.append(pltpu.make_async_copy(wd_h.at[cols, :], wd.at[cols, :], w_sem.at[2, i]))
    first = min(4, n_chunk)
    for i in range(first):
        for c in w_cps[i]:
            c.start()

    lane, tok_id = pos.lanes()
    for c in x_cp:
        c.wait()
    xf = xv[...].astype(F32)
    ssq = jnp.sum(xf * xf, axis=1, keepdims=True)
    st1[pos.hid] = jnp.sum(jnp.where(lane == tok_id, ssq, 0.0), axis=0, keepdims=True)
    pl.semaphore_wait(barrier, len(pos.peers))
    sends = []
    for k, dev in enumerate((pos.core_peer, pos.chip_peer, pos.diag_peer)):
        c = rcopy(st1.at[pos.hid], st1.at[pos.hid], st_ss.at[0, k], st_rs.at[0, pos.hid], {"hid": dev})
        c.start()
        sends.append(c)

    for c in dq_cp:
        c.wait()
    wq_cp.wait()
    for i in range(first, n_chunk):
        for c in w_cps[i]:
            c.start()
    for i in range(n_chunk):
        wd_cps[i].start()
    for c in dx_cp:
        c.start()
    qk = min(768, dqv.shape[1])
    acc[...] = dot_nt(dqv[:, :qk], wq[:, :qk])

    def dn2_body(k, _):
        cols = pl.ds(pl.multiple_of(k * qk, qk), qk)
        acc[...] += dot_nt(dqv[:, cols], wq[:, cols])
        return 0
    lax.fori_loop(1, dqv.shape[1] // qk, dn2_body, 0)
    dn2r[pos.ffn] = acc[...].astype(BF)
    for df in range(1, n_ffn):
        c = rcopy(dn2r.at[pos.ffn], dn2r.at[pos.ffn], z_ss.at[0, df], z_rs.at[0, pos.ffn],
                  {"ffn": (pos.ffn + df) % n_ffn})
        c.start()
        sends.append(c)

    for dev in (pos.core_peer, pos.chip_peer, pos.diag_peer):
        rcopy(st1.at[dev], st1.at[dev], st_ss.at[0, 0], st_rs.at[0, dev], {"hid": dev}).wait_recv()
    tot1 = (st1[0] + st1[1]) + (st1[2] + st1[3])
    mean1 = jnp.sum(jnp.where(lane == tok_id, tot1, 0.0), axis=1, keepdims=True) / d_model
    inv1 = lax.rsqrt(mean1 + NORM_EPS)
    g1v = jnp.reshape(g1_ref[...], (1, width))
    g2v = jnp.reshape(g2_ref[...], (1, width))
    n1 = (xf * inv1 * g1v).astype(BF)
    n1v[...] = n1

    def fwd_a(i):
        for c in w_cps[i]:
            c.wait()
        for w_ref, base in ((wg, 0), (wu, cw)):
            p = dot_nn(n1v[...], w_ref[:, i * cw:(i + 1) * cw])
            own1[i, :, base:base + cw] = p[:half]
            d2s[i, :, base:base + cw] = p[half:]
        c = rcopy(d2s.at[i], d2r.at[i], d2_ss.at[0, i], d2_rs.at[0, i], {"hid": pos.core_peer})
        c.start()
        sends.append(c)

    def fwd_b(i):
        rcopy(d2s.at[i], d2r.at[i], d2_ss.at[0, i], d2_rs.at[0, i], {"hid": pos.core_peer}).wait_recv()
        ys[i] = (own1[i, rows:half] + d2r[i, rows:half]).astype(BF)
        c = rcopy(ys.at[i], yr.at[i], y_ss.at[0, i], y_rs.at[0, i], {"hid": pos.chip_peer})
        c.start()
        sends.append(c)
        gu[i] = own1[i, :rows] + d2r[i, :rows]

    def ag_start(buf, ph, i):
        own = buf.at[i, pl.ds(0, rows)]
        c = rcopy(own, buf.at[i, pl.ds(rows, rows)], ag_ss.at[ph, 0, i], ag_rs.at[ph, 0, i], {"hid": pos.chip_peer})
        c.start()
        sends.append(c)
        c = rcopy(own, buf.at[i, pl.ds(half, rows)], ag_ss.at[ph, 1, i], ag_rs.at[ph, 1, i], {"hid": pos.core_peer})
        c.start()
        sends.append(c)

    def ag_wait(buf, ph, lvl, i):
        blk = buf.at[i, pl.ds((lvl + 1) * rows, rows)]
        rcopy(blk, blk, ag_ss.at[ph, lvl, i], ag_rs.at[ph, lvl, i], {"hid": pos.core_peer}).wait_recv()

    def ag_forward(buf, ph, i):
        ag_wait(buf, ph, 0, i)
        c = rcopy(buf.at[i, pl.ds(rows, rows)], buf.at[i, pl.ds(3 * rows, rows)],
                  ag_ss.at[ph, 2, i], ag_rs.at[ph, 2, i], {"hid": pos.core_peer})
        c.start()
        sends.append(c)

    def fwd_c(i):
        rcopy(ys.at[i], yr.at[i], y_ss.at[0, i], y_rs.at[0, i], {"hid": pos.chip_peer}).wait_recv()
        tot = gu[i] + yr[i].astype(F32)
        gu[i] = tot
        g, u = tot[:, :cw], tot[:, cw:]
        av[i, :rows] = (jax.nn.silu(g) * u).astype(BF)
        ag_start(av, 0, i)

    def fwd_e(i):
        ag_wait(av, 0, 1, i)
        ag_wait(av, 0, 2, i)
        wd_cps[i].wait()
        p = dot_nn(av[i], wd[i * cw:(i + 1) * cw, :])
        if i == 0:
            acc[...] = p
        else:
            acc[...] += p

    def lagged(*stages):
        last = max(lag for _, lag in stages)
        for s in range(n_chunk + last):
            for fn, lag in stages:
                if 0 <= s - lag < n_chunk:
                    fn(s - lag)

    lagged((fwd_a, 0), (fwd_b, 2))
    n1t[...] = jnp.transpose(n1v[...])
    lagged((fwd_c, 0))
    lagged((lambda i: ag_forward(av, 0, i), 0), (fwd_e, 2))

    z_scatter(pos, acc, zs, zr, z_ss.at[1], z_rs.at[1], sends)
    for df in range(1, n_ffn):
        frm = (pos.ffn + df) % n_ffn
        rcopy(dn2r.at[frm], dn2r.at[frm], z_ss.at[0, df], z_rs.at[0, frm], {"ffn": frm}).wait_recv()
    dn2_tot = dn2r[0].astype(F32)
    for s in range(1, n_ffn):
        dn2_tot = dn2_tot + dn2r[s].astype(F32)
    ev[...] = dn2_tot
    my_rows = pos.my_rows()
    x2_rows = (xv[my_rows, :].astype(F32) + z_total(pos, acc, zr, z_ss.at[1], z_rs.at[1])).astype(BF)
    x2v[my_rows, :] = x2_rows
    z_gather(pos, x2v, z_ss.at[2], z_rs.at[2], sends)
    x2_f = x2_rows.astype(F32)
    stat_send(pos, st2, st_ss.at[1], st_rs.at[1],
              jnp.sum(x2_f * x2_f, axis=1, keepdims=True),
              jnp.sum(g2v * x2_f * ev[my_rows, :], axis=1, keepdims=True), sends)
    for c in dx_cp:
        c.wait()
    z_gather_wait(pos, x2v, z_ss.at[2], z_rs.at[2])
    tot2 = stat_total(pos, st2, st_ss.at[1], st_rs.at[1])
    lane, tok_id = pos.lanes()
    inv2 = lax.rsqrt(jnp.sum(jnp.where(lane == tok_id, tot2, 0.0), axis=1, keepdims=True) / d_model + NORM_EPS)
    c2 = jnp.sum(jnp.where(lane == tok_id + tokens, tot2, 0.0), axis=1, keepdims=True)
    x2f = x2v[...].astype(F32)
    dn2 = ev[...]
    e_val = dxv[...].astype(F32) + (inv2 * (g2v * dn2) - x2f * (inv2 ** 3) * (c2 / d_model))
    ev[...] = e_val
    ebv[...] = e_val.astype(BF)
    n2v[...] = (x2f * inv2 * g2v).astype(BF)
    dg2_o[...] = jnp.sum(dn2 * x2f * inv2, axis=0)

    def bwd_a(i):
        p = dot_nt(ebv[...], wd[i * cw:(i + 1) * cw, :])
        own2[i] = p[:half]
        e2s[i] = p[half:]
        c = rcopy(e2s.at[i], e2r.at[i], d2_ss.at[1, i], d2_rs.at[1, i], {"hid": pos.core_peer})
        c.start()
        sends.append(c)

    def bwd_b(i):
        rcopy(e2s.at[i], e2r.at[i], d2_ss.at[1, i], d2_rs.at[1, i], {"hid": pos.core_peer}).wait_recv()
        ys2[i] = (own2[i, rows:half] + e2r[i, rows:half]).astype(BF)
        c = rcopy(ys2.at[i], yr2.at[i], y_ss.at[1, i], y_rs.at[1, i], {"hid": pos.chip_peer})
        c.start()
        sends.append(c)

    def bwd_c(i):
        rcopy(ys2.at[i], yr2.at[i], y_ss.at[1, i], y_rs.at[1, i], {"hid": pos.chip_peer}).wait_recv()
        d_act = own2[i, :rows] + e2r[i, :rows] + yr2[i].astype(F32)
        g, u = gu[i, :, :cw], gu[i, :, cw:]
        sig = jax.nn.sigmoid(g)
        dgu[i, :rows, :cw] = (d_act * u * sig * (1.0 + g * (1.0 - sig))).astype(BF)
        dgu[i, :rows, cw:] = (d_act * (g * sig)).astype(BF)
        ag_start(dgu, 1, i)

    def bwd_e(i):
        ag_wait(dgu, 1, 1, i)
        ag_wait(dgu, 1, 2, i)
        cols = slice(i * cw, (i + 1) * cw)
        p = dot_nt(dgu[i, :, :cw], wg[:, cols]) + dot_nt(dgu[i, :, cw:], wu[:, cols])
        if i == 0:
            acc[...] = p
        else:
            acc[...] += p

    def fill_gate(i):
        cols = slice(i * cw, (i + 1) * cw)
        wg[:, cols] = dot_nn(n1t[...], dgu[i, :, :cw]).astype(BF)
        wu[:, cols] = dot_nn(n1t[...], dgu[i, :, cw:]).astype(BF)

    piece = min(256, cw)

    def fill_down(i):
        for t in range(cw // piece):
            r = i * cw + t * piece
            wd[r:r + piece, :] = dot_tn(av[i, :, t * piece:(t + 1) * piece], ebv[...]).astype(BF)

    qt = dqv.shape[1] // n_chunk

    def fill_qkv(i):
        cols = slice(i * qt, (i + 1) * qt)
        wq[:, cols] = dot_nn(n2t[...], dqv[:, cols]).astype(BF)

    lagged((bwd_a, 0), (bwd_b, 2))
    n2t[...] = jnp.transpose(n2v[...])
    early = n_chunk // 3
    for i in range(early):
        fill_down(i)
    for i in range(n_chunk):
        bwd_c(i)
        if early + i < n_chunk:
            fill_down(early + i)
        if i >= n_chunk // 2:
            fill_qkv(2 * (i - n_chunk // 2))
            fill_qkv(2 * (i - n_chunk // 2) + 1)
    late = n_chunk // 3
    lagged((lambda i: ag_forward(dgu, 1, i), 0), (bwd_e, 1), (lambda i: fill_gate(i - late) if i >= late else None, 1))

    z_scatter(pos, acc, zs2, zr2, z_ss.at[3], z_rs.at[3], sends)
    for i in range(n_chunk - late, n_chunk - late // 2):
        fill_gate(i)
    g1v = jnp.reshape(g1_ref[...], (1, width))
    dn1_rows = z_total(pos, acc, zr2, z_ss.at[3], z_rs.at[3]).astype(BF)
    dn1v[my_rows, :] = dn1_rows
    z_gather(pos, dn1v, z_ss.at[4], z_rs.at[4], sends)
    stat_send(pos, st3, st_ss.at[2], st_rs.at[2], None,
              jnp.sum(g1v * xv[my_rows, :].astype(F32) * dn1_rows.astype(F32), axis=1, keepdims=True), sends)
    for i in range(n_chunk - late // 2, n_chunk):
        fill_gate(i)
    z_gather_wait(pos, dn1v, z_ss.at[4], z_rs.at[4])
    tot3 = stat_total(pos, st3, st_ss.at[2], st_rs.at[2])
    lane, tok_id = pos.lanes()
    c1 = jnp.sum(jnp.where(lane == tok_id + tokens, tot3, 0.0), axis=1, keepdims=True)
    tot1 = (st1[0] + st1[1]) + (st1[2] + st1[3])
    mean1 = jnp.sum(jnp.where(lane == tok_id, tot1, 0.0), axis=1, keepdims=True) / d_model
    inv1 = lax.rsqrt(mean1 + NORM_EPS)
    xf = xv[...].astype(F32)
    dn1 = dn1v[...].astype(F32)
    dx = (ev[...] + (inv1 * (g1v * dn1) - xf * (inv1 ** 3) * (c1 / d_model))).astype(BF)
    for j in range(4):
        dx_o[pl.ds(pl.multiple_of(pos.true_row(j), rows), rows), :] = dx[rows * j:rows * (j + 1)]
    dg1_o[...] = jnp.sum(dn1 * xf * inv1, axis=0)
    for c in sends:
        c.wait_send()


def store_kernel(*refs):
    n_part = 4
    srcs, dsts, sem = refs[:7], refs[7:14], refs[14]
    cps = []
    for k in range(4):
        rows = srcs[k].shape[0] // n_part
        for j in range(n_part):
            cps.append(pltpu.make_async_copy(
                srcs[k].at[pl.ds(j * rows, rows)], dsts[k].at[pl.ds(j * rows, rows)], sem.at[k, j]))
    for k in range(4, 7):
        cps.append(pltpu.make_async_copy(srcs[k], dsts[k], sem.at[k, 0]))
    for c in cps:
        c.start()
    for c in cps:
        c.wait()


def solution(mesh):
    n_hid, n_ffn = mesh.shape["hid"], mesh.shape["ffn"]

    def local_step(x_in, gain_one, gain_two, w_gate, w_up, w_down, w_qkv, dx_out, d_qkv):
        tokens, width = x_in.shape
        ffn_w, qkv_w = w_gate.shape[1], w_qkv.shape[1]
        n_chunk = N_CHUNK
        cw = ffn_w // n_chunk
        rows = tokens // 4
        sds = jax.ShapeDtypeStruct
        vm = pltpu.VMEM
        dma = pltpu.SemaphoreType.DMA
        outs = pl.pallas_call(
            functools.partial(step_kernel, (n_chunk, n_ffn, width * n_hid)),
            out_shape=(
                vm((width, ffn_w), BF), vm((width, ffn_w), BF), vm((ffn_w, width), BF), vm((width, qkv_w), BF),
                vm((tokens, width), BF), vm((width,), F32), vm((width,), F32),
            ),
            in_specs=[ANY, VM, VM] + [ANY] * 6,
            out_specs=(VM,) * 7,
            scratch_shapes=[
                vm((tokens, width), BF), vm((tokens, width), F32), vm((tokens, width), BF), vm((tokens, qkv_w), BF),
                vm((tokens, width), BF), vm((width, tokens), BF), vm((tokens, width), BF), vm((width, tokens), BF),
                vm((tokens, width), BF), vm((tokens, width), F32),
                vm((n_chunk, 2 * rows, 2 * cw), F32), vm((n_chunk, 2 * rows, 2 * cw), F32), vm((n_chunk, 2 * rows, 2 * cw), F32),
                vm((n_chunk, rows, 2 * cw), BF), vm((n_chunk, rows, 2 * cw), BF), vm((n_chunk, rows, 2 * cw), F32),
                vm((n_chunk, tokens, cw), BF),
                vm((n_chunk, 2 * rows, cw), F32), vm((n_chunk, 2 * rows, cw), F32), vm((n_chunk, 2 * rows, cw), F32),
                vm((n_chunk, rows, cw), BF), vm((n_chunk, rows, cw), BF), vm((n_chunk, tokens, 2 * cw), BF),
                vm((n_ffn, tokens, width), BF),
                vm((tokens, width), BF), vm((n_ffn - 1, rows, width), BF), vm((tokens, width), BF),
                vm((tokens, width), BF), vm((n_ffn - 1, rows, width), BF), vm((tokens, width), BF),
                vm((4, 1, LANES), F32), vm((4 * n_ffn, 1, LANES), F32), vm((4 * n_ffn, 1, LANES), F32),
                dma((13,)), dma((3, n_chunk)),
                dma((2, n_chunk)), dma((2, n_chunk)), dma((2, n_chunk)), dma((2, n_chunk)),
                dma((2, 3, n_chunk)), dma((2, 3, n_chunk)), dma((5, n_ffn)), dma((5, n_ffn)),
                dma((3, 4 * n_ffn)), dma((3, 4 * n_ffn)),
            ],
            compiler_params=pltpu.CompilerParams(
                collective_id=0, has_side_effects=True, vmem_limit_bytes=30 * 2 ** 20),
            name="block_step",
        )(x_in, gain_one, gain_two, w_gate, w_up, w_down, w_qkv, dx_out, d_qkv)
        outs = [pltpu.with_memory_space_constraint(o, pltpu.VMEM) for o in outs]
        dw_gate, dw_up, dw_down, dw_qkv, dx_in, dg1, dg2 = pl.pallas_call(
            store_kernel,
            out_shape=tuple(sds(o.shape, o.dtype) for o in outs),
            in_specs=[VM] * 7,
            out_specs=(ANY,) * 7,
            scratch_shapes=[dma((7, 4))],
            compiler_params=pltpu.CompilerParams(vmem_limit_bytes=30 * 2 ** 20),
            name="store_grads",
        )(*outs)
        return dx_in, dw_gate, dw_up, dw_down, dw_qkv, dg1, dg2

    tok_spec = P("data", "hid")
    in_specs = (tok_spec, P("hid"), P("hid"), P("hid", "ffn"), P("hid", "ffn"), P("ffn", "hid"), P("hid", "ffn"), tok_spec, P("data", "ffn"))
    out_specs = (tok_spec, P(("data", "hid"), "ffn"), P(("data", "hid"), "ffn"), P(("data", "ffn"), "hid"), P(("data", "hid"), "ffn"), P(("data", "hid")), P(("data", "hid")))
    return jax.shard_map(local_step, mesh=mesh, in_specs=in_specs, out_specs=out_specs, check_vma=False)
```

```python
import functools
import jax
import jax.numpy as jnp
from jax import lax
from jax.experimental import pallas as pl
from jax.experimental.pallas import tpu as pltpu
from jax.sharding import PartitionSpec as P

NORM_EPS = 1e-6
MESH = pl.DeviceIdType.MESH
ANY = pl.BlockSpec(memory_space=pl.ANY)
VM = pl.BlockSpec(memory_space=pltpu.VMEM)
BF = jnp.bfloat16
F32 = jnp.float32
LANES = 128
N_CHUNK = 6


def dot_nn(a_mat, b_mat):
    return lax.dot_general(a_mat, b_mat, (((1,), (0,)), ((), ())), preferred_element_type=F32)


def dot_nt(a_mat, b_mat):
    return lax.dot_general(a_mat, b_mat, (((1,), (1,)), ((), ())), preferred_element_type=F32)


def dot_tn(a_mat, b_mat):
    return lax.dot_general(a_mat, b_mat, (((0,), (0,)), ((), ())), preferred_element_type=F32)


class Place:
    def __init__(self, tokens, n_ffn):
        self.tokens, self.rows, self.n_ffn = tokens, tokens // 4, n_ffn
        self.hid = lax.axis_index("hid")
        self.ffn = lax.axis_index("ffn")
        self.chip, self.core = self.hid // 2, self.hid % 2
        self.core_peer = 2 * self.chip + (1 - self.core)
        self.chip_peer = 2 * (1 - self.chip) + self.core
        self.diag_peer = 2 * (1 - self.chip) + (1 - self.core)
        self.peers = []
        for dh in range(4):
            for df in range(n_ffn):
                if dh or df:
                    self.peers.append({"hid": (self.hid + dh) % 4, "ffn": (self.ffn + df) % n_ffn})

    def true_row(self, block):
        return self.rows * (2 * ((block // 2 + self.core) % 2) + (block % 2 + self.chip) % 2)

    def my_rows(self, ffn=None):
        return pl.ds(pl.multiple_of(self.rows * (self.ffn if ffn is None else ffn), self.rows), self.rows)

    def lanes(self):
        lane = lax.broadcasted_iota(jnp.int32, (self.tokens, LANES), 1)
        row = lax.broadcasted_iota(jnp.int32, (self.tokens, LANES), 0)
        rows = self.rows
        tok = rows * (2 * ((row // (2 * rows) + self.core) % 2) + ((row // rows) % 2 + self.chip) % 2) + row % rows
        return lane, tok

    def signal_all(self, barrier):
        for dev in self.peers:
            pl.semaphore_signal(barrier, inc=1, device_id=dev, device_id_type=MESH)


def rcopy(src, dst, ss, rs, dev):
    return pltpu.make_async_remote_copy(
        src_ref=src, dst_ref=dst, send_sem=ss, recv_sem=rs, device_id=dev, device_id_type=MESH)


def z_scatter(pos, part, sb, rb, ss, rs, sends):
    sb[...] = part[...].astype(BF)
    for df in range(1, pos.n_ffn):
        to = (pos.ffn + df) % pos.n_ffn
        c = rcopy(sb.at[pos.my_rows(to)], rb.at[df - 1], ss.at[df], rs.at[df], {"ffn": to})
        c.start()
        sends.append(c)


def z_total(pos, part, rb, ss, rs):
    tot = part[pos.my_rows(), :]
    for df in range(1, pos.n_ffn):
        rcopy(rb.at[df - 1], rb.at[df - 1], ss.at[df], rs.at[df], {"ffn": pos.ffn}).wait_recv()
        tot = tot + rb[df - 1].astype(F32)
    return tot


def z_gather(pos, buf, ss, rs, sends):
    mine = buf.at[pos.my_rows()]
    for df in range(1, pos.n_ffn):
        c = rcopy(mine, mine, ss.at[df], rs.at[pos.ffn], {"ffn": (pos.ffn + df) % pos.n_ffn})
        c.start()
        sends.append(c)


def z_gather_wait(pos, buf, ss, rs):
    for df in range(1, pos.n_ffn):
        frm = (pos.ffn + df) % pos.n_ffn
        blk = buf.at[pos.my_rows(frm)]
        rcopy(blk, blk, ss.at[df], rs.at[frm], {"ffn": frm}).wait_recv()


def stat_send(pos, st, ss, rs, ssq_v, c_v, sends):
    ln = lax.broadcasted_iota(jnp.int32, (pos.rows, LANES), 1)
    tid = pos.true_row(pos.ffn) + lax.broadcasted_iota(jnp.int32, (pos.rows, LANES), 0)
    val = jnp.where(ln == tid + pos.tokens, c_v, 0.0)
    if ssq_v is not None:
        val = val + jnp.where(ln == tid, ssq_v, 0.0)
    me = pos.hid * pos.n_ffn + pos.ffn
    st[me] = jnp.sum(val, axis=0, keepdims=True)
    for j, dev in enumerate(pos.peers):
        c = rcopy(st.at[me], st.at[me], ss.at[j], rs.at[me], dev)
        c.start()
        sends.append(c)


def stat_total(pos, st, ss, rs):
    for j, dev in enumerate(pos.peers):
        slot = dev["hid"] * pos.n_ffn + dev["ffn"]
        rcopy(st.at[slot], st.at[slot], ss.at[j], rs.at[slot], dev).wait_recv()
    tot = st[0]
    for s in range(1, 4 * pos.n_ffn):
        tot = tot + st[s]
    return tot


def step_kernel(
    dims,
    x_h, g1_ref, g2_ref, wg_h, wu_h, wd_h, wq_h, dxo_h, dq_h,
    wg, wu, wd, wq, dx_o, dg1_o, dg2_o,
    xv, ev, dxv, dqv, n1v, n1t, n2v, n2t, ebv, acc, own1, d2s, d2r, ys, yr, gu, av,
    own2, e2s, e2r, ys2, yr2, dgu,
    dn2r, zs, zr, x2v, zs2, zr2, dn1v, st1, st2, st3,
    ld_sem, w_sem,
    d2_ss, d2_rs, y_ss, y_rs, ag_ss, ag_rs, z_ss, z_rs, st_ss, st_rs,
):
    n_chunk, n_ffn, d_model = dims
    tokens, width = xv.shape
    rows = tokens // 4
    half = 2 * rows
    ffn_w = wg.shape[1]
    cw = ffn_w // n_chunk
    pos = Place(tokens, n_ffn)
    barrier = pltpu.get_barrier_semaphore()
    pos.signal_all(barrier)

    def load_rows(src, dst, slot):
        cps = []
        for j in range(4):
            r = pl.multiple_of(pos.true_row(j), rows)
            cps.append(pltpu.make_async_copy(
                src.at[pl.ds(r, rows), :], dst.at[pl.ds(rows * j, rows), :], ld_sem.at[slot + j]))
        return cps

    x_cp = load_rows(x_h, xv, 0)
    dq_cp = load_rows(dq_h, dqv, 4)
    dx_cp = load_rows(dxo_h, dxv, 8)
    wq_cp = pltpu.make_async_copy(wq_h, wq, ld_sem.at[12])
    for c in x_cp:
        c.start()
    for c in dq_cp:
        c.start()
    wq_cp.start()
    w_cps, wd_cps = [], []
    for i in range(n_chunk):
        cols = pl.ds(i * cw, cw)
        w_cps.append([
            pltpu.make_async_copy(wg_h.at[:, cols], wg.at[:, cols], w_sem.at[0, i]),
            pltpu.make_async_copy(wu_h.at[:, cols], wu.at[:, cols], w_sem.at[1, i]),
        ])
        wd_cps.append(pltpu.make_async_copy(wd_h.at[cols, :], wd.at[cols, :], w_sem.at[2, i]))
    first = min(4, n_chunk)
    for i in range(first):
        for c in w_cps[i]:
            c.start()

    lane, tok_id = pos.lanes()
    for c in x_cp:
        c.wait()
    xf = xv[...].astype(F32)
    ssq = jnp.sum(xf * xf, axis=1, keepdims=True)
    st1[pos.hid] = jnp.sum(jnp.where(lane == tok_id, ssq, 0.0), axis=0, keepdims=True)
    pl.semaphore_wait(barrier, len(pos.peers))
    sends = []
    for k, dev in enumerate((pos.core_peer, pos.chip_peer, pos.diag_peer)):
        c = rcopy(st1.at[pos.hid], st1.at[pos.hid], st_ss.at[0, k], st_rs.at[0, pos.hid], {"hid": dev})
        c.start()
        sends.append(c)

    for c in dq_cp:
        c.wait()
    wq_cp.wait()
    for i in range(first, n_chunk):
        for c in w_cps[i]:
            c.start()
    for i in range(n_chunk):
        wd_cps[i].start()
    for c in dx_cp:
        c.start()
    qk = min(768, dqv.shape[1])
    acc[...] = dot_nt(dqv[:, :qk], wq[:, :qk])

    def dn2_body(k, _):
        cols = pl.ds(pl.multiple_of(k * qk, qk), qk)
        acc[...] += dot_nt(dqv[:, cols], wq[:, cols])
        return 0
    lax.fori_loop(1, dqv.shape[1] // qk, dn2_body, 0)
    dn2r[pos.ffn] = acc[...].astype(BF)
    for df in range(1, n_ffn):
        c = rcopy(dn2r.at[pos.ffn], dn2r.at[pos.ffn], z_ss.at[0, df], z_rs.at[0, pos.ffn],
                  {"ffn": (pos.ffn + df) % n_ffn})
        c.start()
        sends.append(c)

    for dev in (pos.core_peer, pos.chip_peer, pos.diag_peer):
        rcopy(st1.at[dev], st1.at[dev], st_ss.at[0, 0], st_rs.at[0, dev], {"hid": dev}).wait_recv()
    tot1 = (st1[0] + st1[1]) + (st1[2] + st1[3])
    mean1 = jnp.sum(jnp.where(lane == tok_id, tot1, 0.0), axis=1, keepdims=True) / d_model
    inv1 = lax.rsqrt(mean1 + NORM_EPS)
    g1v = jnp.reshape(g1_ref[...], (1, width))
    g2v = jnp.reshape(g2_ref[...], (1, width))
    n1 = (xf * inv1 * g1v).astype(BF)
    n1v[...] = n1

    def fwd_a(i):
        for c in w_cps[i]:
            c.wait()
        for w_ref, base in ((wg, 0), (wu, cw)):
            p = dot_nn(n1v[...], w_ref[:, i * cw:(i + 1) * cw])
            own1[i, :, base:base + cw] = p[:half]
            d2s[i, :, base:base + cw] = p[half:]
        c = rcopy(d2s.at[i], d2r.at[i], d2_ss.at[0, i], d2_rs.at[0, i], {"hid": pos.core_peer})
        c.start()
        sends.append(c)

    def fwd_b(i):
        rcopy(d2s.at[i], d2r.at[i], d2_ss.at[0, i], d2_rs.at[0, i], {"hid": pos.core_peer}).wait_recv()
        ys[i] = (own1[i, rows:half] + d2r[i, rows:half]).astype(BF)
        c = rcopy(ys.at[i], yr.at[i], y_ss.at[0, i], y_rs.at[0, i], {"hid": pos.chip_peer})
        c.start()
        sends.append(c)
        gu[i] = own1[i, :rows] + d2r[i, :rows]

    def ag_start(buf, ph, i):
        own = buf.at[i, pl.ds(0, rows)]
        c = rcopy(own, buf.at[i, pl.ds(rows, rows)], ag_ss.at[ph, 0, i], ag_rs.at[ph, 0, i], {"hid": pos.chip_peer})
        c.start()
        sends.append(c)
        c = rcopy(own, buf.at[i, pl.ds(half, rows)], ag_ss.at[ph, 1, i], ag_rs.at[ph, 1, i], {"hid": pos.core_peer})
        c.start()
        sends.append(c)

    def ag_wait(buf, ph, lvl, i):
        blk = buf.at[i, pl.ds((lvl + 1) * rows, rows)]
        rcopy(blk, blk, ag_ss.at[ph, lvl, i], ag_rs.at[ph, lvl, i], {"hid": pos.core_peer}).wait_recv()

    def ag_forward(buf, ph, i):
        ag_wait(buf, ph, 0, i)
        c = rcopy(buf.at[i, pl.ds(rows, rows)], buf.at[i, pl.ds(3 * rows, rows)],
                  ag_ss.at[ph, 2, i], ag_rs.at[ph, 2, i], {"hid": pos.core_peer})
        c.start()
        sends.append(c)

    def fwd_c(i):
        rcopy(ys.at[i], yr.at[i], y_ss.at[0, i], y_rs.at[0, i], {"hid": pos.chip_peer}).wait_recv()
        tot = gu[i] + yr[i].astype(F32)
        gu[i] = tot
        g, u = tot[:, :cw], tot[:, cw:]
        av[i, :rows] = (jax.nn.silu(g) * u).astype(BF)
        ag_start(av, 0, i)

    def fwd_e(i):
        ag_wait(av, 0, 1, i)
        ag_wait(av, 0, 2, i)
        wd_cps[i].wait()
        p = dot_nn(av[i], wd[i * cw:(i + 1) * cw, :])
        if i == 0:
            acc[...] = p
        else:
            acc[...] += p

    def lagged(*stages):
        last = max(lag for _, lag in stages)
        for s in range(n_chunk + last):
            for fn, lag in stages:
                if 0 <= s - lag < n_chunk:
                    fn(s - lag)

    lagged((fwd_a, 0), (fwd_b, 2))
    n1t[...] = jnp.transpose(n1v[...])
    lagged((fwd_c, 0))
    lagged((lambda i: ag_forward(av, 0, i), 0), (fwd_e, 2))

    z_scatter(pos, acc, zs, zr, z_ss.at[1], z_rs.at[1], sends)
    for df in range(1, n_ffn):
        frm = (pos.ffn + df) % n_ffn
        rcopy(dn2r.at[frm], dn2r.at[frm], z_ss.at[0, df], z_rs.at[0, frm], {"ffn": frm}).wait_recv()
    dn2_tot = dn2r[0].astype(F32)
    for s in range(1, n_ffn):
        dn2_tot = dn2_tot + dn2r[s].astype(F32)
    ev[...] = dn2_tot
    my_rows = pos.my_rows()
    x2_rows = (xv[my_rows, :].astype(F32) + z_total(pos, acc, zr, z_ss.at[1], z_rs.at[1])).astype(BF)
    x2v[my_rows, :] = x2_rows
    z_gather(pos, x2v, z_ss.at[2], z_rs.at[2], sends)
    x2_f = x2_rows.astype(F32)
    stat_send(pos, st2, st_ss.at[1], st_rs.at[1],
              jnp.sum(x2_f * x2_f, axis=1, keepdims=True),
              jnp.sum(g2v * x2_f * ev[my_rows, :], axis=1, keepdims=True), sends)
    for c in dx_cp:
        c.wait()
    z_gather_wait(pos, x2v, z_ss.at[2], z_rs.at[2])
    tot2 = stat_total(pos, st2, st_ss.at[1], st_rs.at[1])
    lane, tok_id = pos.lanes()
    inv2 = lax.rsqrt(jnp.sum(jnp.where(lane == tok_id, tot2, 0.0), axis=1, keepdims=True) / d_model + NORM_EPS)
    c2 = jnp.sum(jnp.where(lane == tok_id + tokens, tot2, 0.0), axis=1, keepdims=True)
    x2f = x2v[...].astype(F32)
    dn2 = ev[...]
    e_val = dxv[...].astype(F32) + (inv2 * (g2v * dn2) - x2f * (inv2 ** 3) * (c2 / d_model))
    ev[...] = e_val
    ebv[...] = e_val.astype(BF)
    n2v[...] = (x2f * inv2 * g2v).astype(BF)
    dg2_o[...] = jnp.sum(dn2 * x2f * inv2, axis=0)

    def bwd_a(i):
        p = dot_nt(ebv[...], wd[i * cw:(i + 1) * cw, :])
        own2[i] = p[:half]
        e2s[i] = p[half:]
        c = rcopy(e2s.at[i], e2r.at[i], d2_ss.at[1, i], d2_rs.at[1, i], {"hid": pos.core_peer})
        c.start()
        sends.append(c)

    def bwd_b(i):
        rcopy(e2s.at[i], e2r.at[i], d2_ss.at[1, i], d2_rs.at[1, i], {"hid": pos.core_peer}).wait_recv()
        ys2[i] = (own2[i, rows:half] + e2r[i, rows:half]).astype(BF)
        c = rcopy(ys2.at[i], yr2.at[i], y_ss.at[1, i], y_rs.at[1, i], {"hid": pos.chip_peer})
        c.start()
        sends.append(c)

    def bwd_c(i):
        rcopy(ys2.at[i], yr2.at[i], y_ss.at[1, i], y_rs.at[1, i], {"hid": pos.chip_peer}).wait_recv()
        d_act = own2[i, :rows] + e2r[i, :rows] + yr2[i].astype(F32)
        g, u = gu[i, :, :cw], gu[i, :, cw:]
        sig = jax.nn.sigmoid(g)
        dgu[i, :rows, :cw] = (d_act * u * sig * (1.0 + g * (1.0 - sig))).astype(BF)
        dgu[i, :rows, cw:] = (d_act * (g * sig)).astype(BF)
        ag_start(dgu, 1, i)

    def bwd_e(i):
        ag_wait(dgu, 1, 1, i)
        ag_wait(dgu, 1, 2, i)
        cols = slice(i * cw, (i + 1) * cw)
        p = dot_nt(dgu[i, :, :cw], wg[:, cols]) + dot_nt(dgu[i, :, cw:], wu[:, cols])
        if i == 0:
            acc[...] = p
        else:
            acc[...] += p

    def fill_gate(i):
        cols = slice(i * cw, (i + 1) * cw)
        wg[:, cols] = dot_nn(n1t[...], dgu[i, :, :cw]).astype(BF)
        wu[:, cols] = dot_nn(n1t[...], dgu[i, :, cw:]).astype(BF)

    piece = min(256, cw)

    def fill_down(i):
        for t in range(cw // piece):
            r = i * cw + t * piece
            wd[r:r + piece, :] = dot_tn(av[i, :, t * piece:(t + 1) * piece], ebv[...]).astype(BF)

    qt = dqv.shape[1] // n_chunk

    def fill_qkv(i):
        cols = slice(i * qt, (i + 1) * qt)
        wq[:, cols] = dot_nn(n2t[...], dqv[:, cols]).astype(BF)

    lagged((bwd_a, 0), (bwd_b, 2))
    n2t[...] = jnp.transpose(n2v[...])
    early = n_chunk // 3
    for i in range(early):
        fill_down(i)
    for i in range(n_chunk):
        bwd_c(i)
        if early + i < n_chunk:
            fill_down(early + i)
        if i >= n_chunk // 2:
            fill_qkv(2 * (i - n_chunk // 2))
            fill_qkv(2 * (i - n_chunk // 2) + 1)
    late = n_chunk // 3
    lagged((lambda i: ag_forward(dgu, 1, i), 0), (bwd_e, 1), (lambda i: fill_gate(i - late) if i >= late else None, 1))

    z_scatter(pos, acc, zs2, zr2, z_ss.at[3], z_rs.at[3], sends)
    for i in range(n_chunk - late, n_chunk - late // 2):
        fill_gate(i)
    g1v = jnp.reshape(g1_ref[...], (1, width))
    dn1_rows = z_total(pos, acc, zr2, z_ss.at[3], z_rs.at[3]).astype(BF)
    dn1v[my_rows, :] = dn1_rows
    z_gather(pos, dn1v, z_ss.at[4], z_rs.at[4], sends)
    stat_send(pos, st3, st_ss.at[2], st_rs.at[2], None,
              jnp.sum(g1v * xv[my_rows, :].astype(F32) * dn1_rows.astype(F32), axis=1, keepdims=True), sends)
    for i in range(n_chunk - late // 2, n_chunk):
        fill_gate(i)
    z_gather_wait(pos, dn1v, z_ss.at[4], z_rs.at[4])
    tot3 = stat_total(pos, st3, st_ss.at[2], st_rs.at[2])
    lane, tok_id = pos.lanes()
    c1 = jnp.sum(jnp.where(lane == tok_id + tokens, tot3, 0.0), axis=1, keepdims=True)
    tot1 = (st1[0] + st1[1]) + (st1[2] + st1[3])
    mean1 = jnp.sum(jnp.where(lane == tok_id, tot1, 0.0), axis=1, keepdims=True) / d_model
    inv1 = lax.rsqrt(mean1 + NORM_EPS)
    xf = xv[...].astype(F32)
    dn1 = dn1v[...].astype(F32)
    dx = (ev[...] + (inv1 * (g1v * dn1) - xf * (inv1 ** 3) * (c1 / d_model))).astype(BF)
    for j in range(4):
        dx_o[pl.ds(pl.multiple_of(pos.true_row(j), rows), rows), :] = dx[rows * j:rows * (j + 1)]
    dg1_o[...] = jnp.sum(dn1 * xf * inv1, axis=0)
    for c in sends:
        c.wait_send()


def store_kernel(*refs):
    n_part = 4
    srcs, dsts, sem = refs[:7], refs[7:14], refs[14]
    cps = []
    for k in range(4):
        rows = srcs[k].shape[0] // n_part
        for j in range(n_part):
            cps.append(pltpu.make_async_copy(
                srcs[k].at[pl.ds(j * rows, rows)], dsts[k].at[pl.ds(j * rows, rows)], sem.at[k, j]))
    for k in range(4, 7):
        cps.append(pltpu.make_async_copy(srcs[k], dsts[k], sem.at[k, 0]))
    for c in cps:
        c.start()
    for c in cps:
        c.wait()


def solution(mesh):
    n_hid, n_ffn = mesh.shape["hid"], mesh.shape["ffn"]

    def local_step(x_in, gain_one, gain_two, w_gate, w_up, w_down, w_qkv, dx_out, d_qkv):
        tokens, width = x_in.shape
        ffn_w, qkv_w = w_gate.shape[1], w_qkv.shape[1]
        n_chunk = N_CHUNK
        cw = ffn_w // n_chunk
        rows = tokens // 4
        sds = jax.ShapeDtypeStruct
        vm = pltpu.VMEM
        dma = pltpu.SemaphoreType.DMA
        outs = pl.pallas_call(
            functools.partial(step_kernel, (n_chunk, n_ffn, width * n_hid)),
            out_shape=(
                vm((width, ffn_w), BF), vm((width, ffn_w), BF), vm((ffn_w, width), BF), vm((width, qkv_w), BF),
                vm((tokens, width), BF), vm((width,), F32), vm((width,), F32),
            ),
            in_specs=[ANY, VM, VM] + [ANY] * 6,
            out_specs=(VM,) * 7,
            scratch_shapes=[
                vm((tokens, width), BF), vm((tokens, width), F32), vm((tokens, width), BF), vm((tokens, qkv_w), BF),
                vm((tokens, width), BF), vm((width, tokens), BF), vm((tokens, width), BF), vm((width, tokens), BF),
                vm((tokens, width), BF), vm((tokens, width), F32),
                vm((n_chunk, 2 * rows, 2 * cw), F32), vm((n_chunk, 2 * rows, 2 * cw), F32), vm((n_chunk, 2 * rows, 2 * cw), F32),
                vm((n_chunk, rows, 2 * cw), BF), vm((n_chunk, rows, 2 * cw), BF), vm((n_chunk, rows, 2 * cw), F32),
                vm((n_chunk, tokens, cw), BF),
                vm((n_chunk, 2 * rows, cw), F32), vm((n_chunk, 2 * rows, cw), F32), vm((n_chunk, 2 * rows, cw), F32),
                vm((n_chunk, rows, cw), BF), vm((n_chunk, rows, cw), BF), vm((n_chunk, tokens, 2 * cw), BF),
                vm((n_ffn, tokens, width), BF),
                vm((tokens, width), BF), vm((n_ffn - 1, rows, width), BF), vm((tokens, width), BF),
                vm((tokens, width), BF), vm((n_ffn - 1, rows, width), BF), vm((tokens, width), BF),
                vm((4, 1, LANES), F32), vm((4 * n_ffn, 1, LANES), F32), vm((4 * n_ffn, 1, LANES), F32),
                dma((13,)), dma((3, n_chunk)),
                dma((2, n_chunk)), dma((2, n_chunk)), dma((2, n_chunk)), dma((2, n_chunk)),
                dma((2, 3, n_chunk)), dma((2, 3, n_chunk)), dma((5, n_ffn)), dma((5, n_ffn)),
                dma((3, 4 * n_ffn)), dma((3, 4 * n_ffn)),
            ],
            compiler_params=pltpu.CompilerParams(
                collective_id=0, has_side_effects=True, vmem_limit_bytes=30 * 2 ** 20),
            name="block_step",
        )(x_in, gain_one, gain_two, w_gate, w_up, w_down, w_qkv, dx_out, d_qkv)
        outs = [pltpu.with_memory_space_constraint(o, pltpu.VMEM) for o in outs]
        dw_gate, dw_up, dw_down, dw_qkv, dx_in, dg1, dg2 = pl.pallas_call(
            store_kernel,
            out_shape=tuple(sds(o.shape, o.dtype) for o in outs),
            in_specs=[VM] * 7,
            out_specs=(ANY,) * 7,
            scratch_shapes=[dma((7, 4))],
            compiler_params=pltpu.CompilerParams(vmem_limit_bytes=30 * 2 ** 20),
            name="store_grads",
        )(*outs)
        return dx_in, dw_gate, dw_up, dw_down, dw_qkv, dg1, dg2

    tok_spec = P("data", "hid")
    in_specs = (tok_spec, P("hid"), P("hid"), P("hid", "ffn"), P("hid", "ffn"), P("ffn", "hid"), P("hid", "ffn"), tok_spec, P("data", "ffn"))
    out_specs = (tok_spec, P(("data", "hid"), "ffn"), P(("data", "hid"), "ffn"), P(("data", "ffn"), "hid"), P(("data", "hid"), "ffn"), P(("data", "hid")), P(("data", "hid")))
    return jax.shard_map(local_step, mesh=mesh, in_specs=in_specs, out_specs=out_specs, check_vma=False)
```

```python
import functools
import jax
import jax.numpy as jnp
from jax import lax
from jax.experimental import pallas as pl
from jax.experimental.pallas import tpu as pltpu
from jax.sharding import PartitionSpec as P

NORM_EPS = 1e-6
MESH = pl.DeviceIdType.MESH
ANY = pl.BlockSpec(memory_space=pl.ANY)
VM = pl.BlockSpec(memory_space=pltpu.VMEM)
BF = jnp.bfloat16
F32 = jnp.float32
LANES = 128
N_CHUNK = 6


def dot_nn(a_mat, b_mat):
    return lax.dot_general(a_mat, b_mat, (((1,), (0,)), ((), ())), preferred_element_type=F32)


def dot_nt(a_mat, b_mat):
    return lax.dot_general(a_mat, b_mat, (((1,), (1,)), ((), ())), preferred_element_type=F32)


def dot_tn(a_mat, b_mat):
    return lax.dot_general(a_mat, b_mat, (((0,), (0,)), ((), ())), preferred_element_type=F32)


class Place:
    def __init__(self, tokens, n_ffn):
        self.tokens, self.rows, self.n_ffn = tokens, tokens // 4, n_ffn
        self.hid = lax.axis_index("hid")
        self.ffn = lax.axis_index("ffn")
        self.chip, self.core = self.hid // 2, self.hid % 2
        self.core_peer = 2 * self.chip + (1 - self.core)
        self.chip_peer = 2 * (1 - self.chip) + self.core
        self.diag_peer = 2 * (1 - self.chip) + (1 - self.core)
        self.peers = []
        for dh in range(4):
            for df in range(n_ffn):
                if dh or df:
                    self.peers.append({"hid": (self.hid + dh) % 4, "ffn": (self.ffn + df) % n_ffn})

    def true_row(self, block):
        return self.rows * (2 * ((block // 2 + self.core) % 2) + (block % 2 + self.chip) % 2)

    def my_rows(self, ffn=None):
        return pl.ds(pl.multiple_of(self.rows * (self.ffn if ffn is None else ffn), self.rows), self.rows)

    def lanes(self):
        lane = lax.broadcasted_iota(jnp.int32, (self.tokens, LANES), 1)
        row = lax.broadcasted_iota(jnp.int32, (self.tokens, LANES), 0)
        rows = self.rows
        tok = rows * (2 * ((row // (2 * rows) + self.core) % 2) + ((row // rows) % 2 + self.chip) % 2) + row % rows
        return lane, tok

    def signal_all(self, barrier):
        for dev in self.peers:
            pl.semaphore_signal(barrier, inc=1, device_id=dev, device_id_type=MESH)


def rcopy(src, dst, ss, rs, dev):
    return pltpu.make_async_remote_copy(
        src_ref=src, dst_ref=dst, send_sem=ss, recv_sem=rs, device_id=dev, device_id_type=MESH)


def z_scatter(pos, part, sb, rb, ss, rs, sends):
    sb[...] = part[...].astype(BF)
    for df in range(1, pos.n_ffn):
        to = (pos.ffn + df) % pos.n_ffn
        c = rcopy(sb.at[pos.my_rows(to)], rb.at[df - 1], ss.at[df], rs.at[df], {"ffn": to})
        c.start()
        sends.append(c)


def z_total(pos, part, rb, ss, rs):
    tot = part[pos.my_rows(), :]
    for df in range(1, pos.n_ffn):
        rcopy(rb.at[df - 1], rb.at[df - 1], ss.at[df], rs.at[df], {"ffn": pos.ffn}).wait_recv()
        tot = tot + rb[df - 1].astype(F32)
    return tot


def z_gather(pos, buf, ss, rs, sends):
    mine = buf.at[pos.my_rows()]
    for df in range(1, pos.n_ffn):
        c = rcopy(mine, mine, ss.at[df], rs.at[pos.ffn], {"ffn": (pos.ffn + df) % pos.n_ffn})
        c.start()
        sends.append(c)


def z_gather_wait(pos, buf, ss, rs):
    for df in range(1, pos.n_ffn):
        frm = (pos.ffn + df) % pos.n_ffn
        blk = buf.at[pos.my_rows(frm)]
        rcopy(blk, blk, ss.at[df], rs.at[frm], {"ffn": frm}).wait_recv()


def stat_send(pos, st, ss, rs, ssq_v, c_v, sends):
    ln = lax.broadcasted_iota(jnp.int32, (pos.rows, LANES), 1)
    tid = pos.true_row(pos.ffn) + lax.broadcasted_iota(jnp.int32, (pos.rows, LANES), 0)
    val = jnp.where(ln == tid + pos.tokens, c_v, 0.0)
    if ssq_v is not None:
        val = val + jnp.where(ln == tid, ssq_v, 0.0)
    me = pos.hid * pos.n_ffn + pos.ffn
    st[me] = jnp.sum(val, axis=0, keepdims=True)
    for j, dev in enumerate(pos.peers):
        c = rcopy(st.at[me], st.at[me], ss.at[j], rs.at[me], dev)
        c.start()
        sends.append(c)


def stat_total(pos, st, ss, rs):
    for j, dev in enumerate(pos.peers):
        slot = dev["hid"] * pos.n_ffn + dev["ffn"]
        rcopy(st.at[slot], st.at[slot], ss.at[j], rs.at[slot], dev).wait_recv()
    tot = st[0]
    for s in range(1, 4 * pos.n_ffn):
        tot = tot + st[s]
    return tot


def step_kernel(
    dims,
    x_h, g1_h, g2_h, wg_h, wu_h, wd_h, wq_h, dxo_h, dq_h,
    wg, wu, wd, wq, dx_o, dg1_o, dg2_o,
    g1_ref, g2_ref, xv, ev, dxv, dqv, n1v, n1t, n2v, n2t, ebv, acc, own1, d2s, d2r, ys, yr, gu, av,
    own2, e2s, e2r, ys2, yr2, dgu, pq, dav,
    dn2r, zs, zr, x2v, zs2, zr2, dn1v, st1, st2, st3,
    ld_sem, w_sem,
    d2_ss, d2_rs, y_ss, y_rs, ag_ss, ag_rs, z_ss, z_rs, st_ss, st_rs,
):
    n_chunk, n_ffn, d_model = dims
    tokens, width = xv.shape
    rows = tokens // 4
    half = 2 * rows
    ffn_w = wg.shape[1]
    cw = ffn_w // n_chunk
    pos = Place(tokens, n_ffn)
    barrier = pltpu.get_barrier_semaphore()
    pos.signal_all(barrier)

    def load_rows(src, dst, slot):
        cps = []
        for j in range(4):
            r = pl.multiple_of(pos.true_row(j), rows)
            cps.append(pltpu.make_async_copy(
                src.at[pl.ds(r, rows), :], dst.at[pl.ds(rows * j, rows), :], ld_sem.at[slot + j]))
        return cps

    x_cp = load_rows(x_h, xv, 0)
    dq_cp = load_rows(dq_h, dqv, 4)
    dx_cp = load_rows(dxo_h, dxv, 8)
    wq_cp = pltpu.make_async_copy(wq_h, wq, ld_sem.at[12])
    g_cp = [pltpu.make_async_copy(g1_h, g1_ref, ld_sem.at[13]), pltpu.make_async_copy(g2_h, g2_ref, ld_sem.at[14])]
    for c in x_cp + g_cp:
        c.start()
    for c in dq_cp:
        c.start()
    wq_cp.start()
    w_cps, wd_cps = [], []
    for i in range(n_chunk):
        cols = pl.ds(i * cw, cw)
        w_cps.append([
            pltpu.make_async_copy(wg_h.at[:, cols], wg.at[:, cols], w_sem.at[0, i]),
            pltpu.make_async_copy(wu_h.at[:, cols], wu.at[:, cols], w_sem.at[1, i]),
        ])
        wd_cps.append(pltpu.make_async_copy(wd_h.at[cols, :], wd.at[cols, :], w_sem.at[2, i]))
    first = min(4, n_chunk)
    for i in range(first):
        for c in w_cps[i]:
            c.start()

    lane, tok_id = pos.lanes()
    for c in x_cp:
        c.wait()
    xf = xv[...].astype(F32)
    ssq = jnp.sum(xf * xf, axis=1, keepdims=True)
    st1[pos.hid] = jnp.sum(jnp.where(lane == tok_id, ssq, 0.0), axis=0, keepdims=True)
    pl.semaphore_wait(barrier, len(pos.peers))
    sends = []
    for k, dev in enumerate((pos.core_peer, pos.chip_peer, pos.diag_peer)):
        c = rcopy(st1.at[pos.hid], st1.at[pos.hid], st_ss.at[0, k], st_rs.at[0, pos.hid], {"hid": dev})
        c.start()
        sends.append(c)

    for c in dq_cp:
        c.wait()
    wq_cp.wait()
    for i in range(first, n_chunk):
        for c in w_cps[i]:
            c.start()
    for i in range(n_chunk):
        wd_cps[i].start()
    for c in dx_cp:
        c.start()
    qk = min(768, dqv.shape[1])
    acc[...] = dot_nt(dqv[:, :qk], wq[:, :qk])

    def dn2_body(k, _):
        cols = pl.ds(pl.multiple_of(k * qk, qk), qk)
        acc[...] += dot_nt(dqv[:, cols], wq[:, cols])
        return 0
    lax.fori_loop(1, dqv.shape[1] // qk, dn2_body, 0)
    dn2r[pos.ffn] = acc[...].astype(BF)
    for df in range(1, n_ffn):
        c = rcopy(dn2r.at[pos.ffn], dn2r.at[pos.ffn], z_ss.at[0, df], z_rs.at[0, pos.ffn],
                  {"ffn": (pos.ffn + df) % n_ffn})
        c.start()
        sends.append(c)

    for dev in (pos.core_peer, pos.chip_peer, pos.diag_peer):
        rcopy(st1.at[dev], st1.at[dev], st_ss.at[0, 0], st_rs.at[0, dev], {"hid": dev}).wait_recv()
    tot1 = (st1[0] + st1[1]) + (st1[2] + st1[3])
    mean1 = jnp.sum(jnp.where(lane == tok_id, tot1, 0.0), axis=1, keepdims=True) / d_model
    inv1 = lax.rsqrt(mean1 + NORM_EPS)
    for c in g_cp:
        c.wait()
    g1v = jnp.reshape(g1_ref[...], (1, width))
    g2v = jnp.reshape(g2_ref[...], (1, width))
    n1 = (xf * inv1 * g1v).astype(BF)
    n1v[...] = n1

    def fwd_a(i):
        for c in w_cps[i]:
            c.wait()
        for w_ref, base in ((wg, 0), (wu, cw)):
            p = dot_nn(n1v[...], w_ref[:, i * cw:(i + 1) * cw])
            own1[i, :, base:base + cw] = p[:half]
            d2s[i, :, base:base + cw] = p[half:]
        c = rcopy(d2s.at[i], d2r.at[i], d2_ss.at[0, i], d2_rs.at[0, i], {"hid": pos.core_peer})
        c.start()
        sends.append(c)

    def fwd_b(i):
        rcopy(d2s.at[i], d2r.at[i], d2_ss.at[0, i], d2_rs.at[0, i], {"hid": pos.core_peer}).wait_recv()
        ys[i] = (own1[i, rows:half] + d2r[i, rows:half]).astype(BF)
        c = rcopy(ys.at[i], yr.at[i], y_ss.at[0, i], y_rs.at[0, i], {"hid": pos.chip_peer})
        c.start()
        sends.append(c)
        gu[i] = own1[i, :rows] + d2r[i, :rows]

    def ag_chip(buf, ph, i):
        c = rcopy(buf.at[i, pl.ds(0, rows)], buf.at[i, pl.ds(rows, rows)],
                  ag_ss.at[ph, 0, i], ag_rs.at[ph, 0, i], {"hid": pos.chip_peer})
        c.start()
        sends.append(c)

    def ag_core(buf, ph, i):
        c = rcopy(buf.at[i, pl.ds(0, rows)], buf.at[i, pl.ds(half, rows)],
                  ag_ss.at[ph, 1, i], ag_rs.at[ph, 1, i], {"hid": pos.core_peer})
        c.start()
        sends.append(c)

    def ag_wait(buf, ph, lvl, i):
        blk = buf.at[i, pl.ds((lvl + 1) * rows, rows)]
        rcopy(blk, blk, ag_ss.at[ph, lvl, i], ag_rs.at[ph, lvl, i], {"hid": pos.core_peer}).wait_recv()

    def ag_forward(buf, ph, i):
        ag_wait(buf, ph, 0, i)
        c = rcopy(buf.at[i, pl.ds(rows, rows)], buf.at[i, pl.ds(3 * rows, rows)],
                  ag_ss.at[ph, 2, i], ag_rs.at[ph, 2, i], {"hid": pos.core_peer})
        c.start()
        sends.append(c)

    def fwd_c(i):
        rcopy(ys.at[i], yr.at[i], y_ss.at[0, i], y_rs.at[0, i], {"hid": pos.chip_peer}).wait_recv()
        tot = gu[i] + yr[i].astype(F32)
        g, u = tot[:, :cw], tot[:, cw:]
        sig = jax.nn.sigmoid(g)
        act = g * sig
        av[i, :rows] = (act * u).astype(BF)
        ag_chip(av, 0, i)
        ag_core(av, 0, i)
        pq[i, :rows, :cw] = (u * sig * (1.0 + g * (1.0 - sig))).astype(BF)
        pq[i, :rows, cw:] = act.astype(BF)

    def fwd_e(i):
        ag_wait(av, 0, 1, i)
        ag_wait(av, 0, 2, i)
        wd_cps[i].wait()
        p = dot_nn(av[i], wd[i * cw:(i + 1) * cw, :])
        if i == 0:
            acc[...] = p
        else:
            acc[...] += p

    def lagged(*stages):
        last = max(lag for _, lag in stages)
        for s in range(n_chunk + last):
            for fn, lag in stages:
                if 0 <= s - lag < n_chunk:
                    fn(s - lag)

    lagged((fwd_a, 0), (fwd_b, 2))
    n1t[...] = jnp.transpose(n1v[...])
    lagged((fwd_c, 0))
    ahead = (2 * n_chunk) // 3
    for i in range(ahead):
        ag_chip(pq, 1, i)
    lagged((lambda i: ag_forward(av, 0, i), 0), (fwd_e, 2))

    z_scatter(pos, acc, zs, zr, z_ss.at[1], z_rs.at[1], sends)
    for i in range(n_chunk):
        ag_core(pq, 1, i)
    for df in range(1, n_ffn):
        frm = (pos.ffn + df) % n_ffn
        rcopy(dn2r.at[frm], dn2r.at[frm], z_ss.at[0, df], z_rs.at[0, frm], {"ffn": frm}).wait_recv()
    dn2_tot = dn2r[0].astype(F32)
    for s in range(1, n_ffn):
        dn2_tot = dn2_tot + dn2r[s].astype(F32)
    ev[...] = dn2_tot
    my_rows = pos.my_rows()
    x2_rows = (xv[my_rows, :].astype(F32) + z_total(pos, acc, zr, z_ss.at[1], z_rs.at[1])).astype(BF)
    x2v[my_rows, :] = x2_rows
    z_gather(pos, x2v, z_ss.at[2], z_rs.at[2], sends)
    x2_f = x2_rows.astype(F32)
    stat_send(pos, st2, st_ss.at[1], st_rs.at[1],
              jnp.sum(x2_f * x2_f, axis=1, keepdims=True),
              jnp.sum(g2v * x2_f * ev[my_rows, :], axis=1, keepdims=True), sends)
    for i in range(ahead, n_chunk):
        ag_chip(pq, 1, i)
    for c in dx_cp:
        c.wait()
    z_gather_wait(pos, x2v, z_ss.at[2], z_rs.at[2])
    tot2 = stat_total(pos, st2, st_ss.at[1], st_rs.at[1])
    lane, tok_id = pos.lanes()
    inv2 = lax.rsqrt(jnp.sum(jnp.where(lane == tok_id, tot2, 0.0), axis=1, keepdims=True) / d_model + NORM_EPS)
    c2 = jnp.sum(jnp.where(lane == tok_id + tokens, tot2, 0.0), axis=1, keepdims=True)
    x2f = x2v[...].astype(F32)
    dn2 = ev[...]
    e_val = dxv[...].astype(F32) + (inv2 * (g2v * dn2) - x2f * (inv2 ** 3) * (c2 / d_model))
    ev[...] = e_val
    ebv[...] = e_val.astype(BF)
    n2v[...] = (x2f * inv2 * g2v).astype(BF)
    dg2_o[...] = jnp.sum(dn2 * x2f * inv2, axis=0)

    def bwd_a(i):
        p = dot_nt(ebv[...], wd[i * cw:(i + 1) * cw, :])
        own2[i] = p[:half]
        e2s[i] = p[half:]
        c = rcopy(e2s.at[i], e2r.at[i], d2_ss.at[1, i], d2_rs.at[1, i], {"hid": pos.core_peer})
        c.start()
        sends.append(c)

    def bwd_b(i):
        rcopy(e2s.at[i], e2r.at[i], d2_ss.at[1, i], d2_rs.at[1, i], {"hid": pos.core_peer}).wait_recv()
        ys2[i] = (own2[i, rows:half] + e2r[i, rows:half]).astype(BF)
        c = rcopy(ys2.at[i], yr2.at[i], y_ss.at[1, i], y_rs.at[1, i], {"hid": pos.chip_peer})
        c.start()
        sends.append(c)

    def bwd_c(i):
        rcopy(ys2.at[i], yr2.at[i], y_ss.at[1, i], y_rs.at[1, i], {"hid": pos.chip_peer}).wait_recv()
        d_act = own2[i, :rows] + e2r[i, :rows] + yr2[i].astype(F32)
        dav[i, :rows] = d_act.astype(BF)
        ag_chip(dav, 2, i)
        ag_core(dav, 2, i)

    def bwd_e(i):
        ag_wait(pq, 1, 1, i)
        ag_wait(pq, 1, 2, i)
        ag_wait(dav, 2, 1, i)
        ag_wait(dav, 2, 2, i)
        d_act = dav[i].astype(F32)
        dgu[i, :, :cw] = (d_act * pq[i, :, :cw].astype(F32)).astype(BF)
        dgu[i, :, cw:] = (d_act * pq[i, :, cw:].astype(F32)).astype(BF)
        cols = slice(i * cw, (i + 1) * cw)
        p = dot_nt(dgu[i, :, :cw], wg[:, cols]) + dot_nt(dgu[i, :, cw:], wu[:, cols])
        if i == 0:
            acc[...] = p
        else:
            acc[...] += p

    def fill_gate(i):
        cols = slice(i * cw, (i + 1) * cw)
        wg[:, cols] = dot_nn(n1t[...], dgu[i, :, :cw]).astype(BF)
        wu[:, cols] = dot_nn(n1t[...], dgu[i, :, cw:]).astype(BF)

    piece = min(256, cw)

    def fill_down(i):
        for t in range(cw // piece):
            r = i * cw + t * piece
            wd[r:r + piece, :] = dot_tn(av[i, :, t * piece:(t + 1) * piece], ebv[...]).astype(BF)

    qt = dqv.shape[1] // n_chunk

    def fill_qkv(i):
        cols = slice(i * qt, (i + 1) * qt)
        wq[:, cols] = dot_nn(n2t[...], dqv[:, cols]).astype(BF)

    lagged((bwd_a, 0), (bwd_b, 2))
    for i in range(n_chunk):
        ag_forward(pq, 1, i)
    n2t[...] = jnp.transpose(n2v[...])
    early = n_chunk // 3
    for i in range(early):
        fill_down(i)
    for i in range(n_chunk):
        bwd_c(i)
        if early + i < n_chunk:
            fill_down(early + i)
        if i >= n_chunk // 2:
            fill_qkv(2 * (i - n_chunk // 2))
            fill_qkv(2 * (i - n_chunk // 2) + 1)
    lagged((lambda i: ag_forward(dav, 2, i), 0), (bwd_e, 1))

    z_scatter(pos, acc, zs2, zr2, z_ss.at[3], z_rs.at[3], sends)
    for i in range(n_chunk // 2):
        fill_gate(i)
    g1v = jnp.reshape(g1_ref[...], (1, width))
    dn1_rows = z_total(pos, acc, zr2, z_ss.at[3], z_rs.at[3]).astype(BF)
    dn1v[my_rows, :] = dn1_rows
    z_gather(pos, dn1v, z_ss.at[4], z_rs.at[4], sends)
    stat_send(pos, st3, st_ss.at[2], st_rs.at[2], None,
              jnp.sum(g1v * xv[my_rows, :].astype(F32) * dn1_rows.astype(F32), axis=1, keepdims=True), sends)
    for i in range(n_chunk // 2, n_chunk):
        fill_gate(i)
    z_gather_wait(pos, dn1v, z_ss.at[4], z_rs.at[4])
    tot3 = stat_total(pos, st3, st_ss.at[2], st_rs.at[2])
    lane, tok_id = pos.lanes()
    c1 = jnp.sum(jnp.where(lane == tok_id + tokens, tot3, 0.0), axis=1, keepdims=True)
    tot1 = (st1[0] + st1[1]) + (st1[2] + st1[3])
    mean1 = jnp.sum(jnp.where(lane == tok_id, tot1, 0.0), axis=1, keepdims=True) / d_model
    inv1 = lax.rsqrt(mean1 + NORM_EPS)
    xf = xv[...].astype(F32)
    dn1 = dn1v[...].astype(F32)
    dx = (ev[...] + (inv1 * (g1v * dn1) - xf * (inv1 ** 3) * (c1 / d_model))).astype(BF)
    for j in range(4):
        dx_o[pl.ds(pl.multiple_of(pos.true_row(j), rows), rows), :] = dx[rows * j:rows * (j + 1)]
    dg1_o[...] = jnp.sum(dn1 * xf * inv1, axis=0)
    for c in sends:
        c.wait_send()


def store_kernel(*refs):
    n_part = 4
    srcs, dsts, sem = refs[:7], refs[7:14], refs[14]
    cps = []
    for k in range(4):
        rows = srcs[k].shape[0] // n_part
        for j in range(n_part):
            cps.append(pltpu.make_async_copy(
                srcs[k].at[pl.ds(j * rows, rows)], dsts[k].at[pl.ds(j * rows, rows)], sem.at[k, j]))
    for k in range(4, 7):
        cps.append(pltpu.make_async_copy(srcs[k], dsts[k], sem.at[k, 0]))
    for c in cps:
        c.start()
    for c in cps:
        c.wait()


def solution(mesh):
    n_hid, n_ffn = mesh.shape["hid"], mesh.shape["ffn"]

    def local_step(x_in, gain_one, gain_two, w_gate, w_up, w_down, w_qkv, dx_out, d_qkv):
        tokens, width = x_in.shape
        ffn_w, qkv_w = w_gate.shape[1], w_qkv.shape[1]
        n_chunk = N_CHUNK
        cw = ffn_w // n_chunk
        rows = tokens // 4
        sds = jax.ShapeDtypeStruct
        vm = pltpu.VMEM
        dma = pltpu.SemaphoreType.DMA
        outs = pl.pallas_call(
            functools.partial(step_kernel, (n_chunk, n_ffn, width * n_hid)),
            out_shape=(
                vm((width, ffn_w), BF), vm((width, ffn_w), BF), vm((ffn_w, width), BF), vm((width, qkv_w), BF),
                vm((tokens, width), BF), vm((width,), F32), vm((width,), F32),
            ),
            in_specs=[ANY] * 9,
            out_specs=(VM,) * 7,
            scratch_shapes=[
                vm((width,), F32), vm((width,), F32), vm((tokens, width), BF), vm((tokens, width), F32), vm((tokens, width), BF), vm((tokens, qkv_w), BF),
                vm((tokens, width), BF), vm((width, tokens), BF), vm((tokens, width), BF), vm((width, tokens), BF),
                vm((tokens, width), BF), vm((tokens, width), F32),
                vm((n_chunk, 2 * rows, 2 * cw), F32), vm((n_chunk, 2 * rows, 2 * cw), F32), vm((n_chunk, 2 * rows, 2 * cw), F32),
                vm((n_chunk, rows, 2 * cw), BF), vm((n_chunk, rows, 2 * cw), BF), vm((n_chunk, rows, 2 * cw), F32),
                vm((n_chunk, tokens, cw), BF),
                vm((n_chunk, 2 * rows, cw), F32), vm((n_chunk, 2 * rows, cw), F32), vm((n_chunk, 2 * rows, cw), F32),
                vm((n_chunk, rows, cw), BF), vm((n_chunk, rows, cw), BF), vm((n_chunk, tokens, 2 * cw), BF),
                vm((n_chunk, tokens, 2 * cw), BF), vm((n_chunk, tokens, cw), BF),
                vm((n_ffn, tokens, width), BF),
                vm((tokens, width), BF), vm((n_ffn - 1, rows, width), BF), vm((tokens, width), BF),
                vm((tokens, width), BF), vm((n_ffn - 1, rows, width), BF), vm((tokens, width), BF),
                vm((4, 1, LANES), F32), vm((4 * n_ffn, 1, LANES), F32), vm((4 * n_ffn, 1, LANES), F32),
                dma((15,)), dma((3, n_chunk)),
                dma((2, n_chunk)), dma((2, n_chunk)), dma((2, n_chunk)), dma((2, n_chunk)),
                dma((3, 3, n_chunk)), dma((3, 3, n_chunk)), dma((5, n_ffn)), dma((5, n_ffn)),
                dma((3, 4 * n_ffn)), dma((3, 4 * n_ffn)),
            ],
            compiler_params=pltpu.CompilerParams(
                collective_id=0, has_side_effects=True, vmem_limit_bytes=30 * 2 ** 20),
            name="block_step",
        )(x_in, gain_one, gain_two, w_gate, w_up, w_down, w_qkv, dx_out, d_qkv)
        outs = [pltpu.with_memory_space_constraint(o, pltpu.VMEM) for o in outs]
        dw_gate, dw_up, dw_down, dw_qkv, dx_in, dg1, dg2 = pl.pallas_call(
            store_kernel,
            out_shape=tuple(sds(o.shape, o.dtype) for o in outs),
            in_specs=[VM] * 7,
            out_specs=(ANY,) * 7,
            scratch_shapes=[dma((7, 4))],
            compiler_params=pltpu.CompilerParams(vmem_limit_bytes=30 * 2 ** 20),
            name="store_grads",
        )(*outs)
        return dx_in, dw_gate, dw_up, dw_down, dw_qkv, dg1, dg2

    tok_spec = P("data", "hid")
    in_specs = (tok_spec, P("hid"), P("hid"), P("hid", "ffn"), P("hid", "ffn"), P("ffn", "hid"), P("hid", "ffn"), tok_spec, P("data", "ffn"))
    out_specs = (tok_spec, P(("data", "hid"), "ffn"), P(("data", "hid"), "ffn"), P(("data", "ffn"), "hid"), P(("data", "hid"), "ffn"), P(("data", "hid")), P(("data", "hid")))
    return jax.shard_map(local_step, mesh=mesh, in_specs=in_specs, out_specs=out_specs, check_vma=False)
```

```python
import functools
import jax
import jax.numpy as jnp
from jax import lax
from jax.experimental import pallas as pl
from jax.experimental.pallas import tpu as pltpu
from jax.sharding import PartitionSpec as P

NORM_EPS = 1e-6
MESH = pl.DeviceIdType.MESH
ANY = pl.BlockSpec(memory_space=pl.ANY)
VM = pl.BlockSpec(memory_space=pltpu.VMEM)
BF = jnp.bfloat16
F32 = jnp.float32
LANES = 128
N_CHUNK = 6
N_LATE = 4


def dot_nn(a_mat, b_mat):
    return lax.dot_general(a_mat, b_mat, (((1,), (0,)), ((), ())), preferred_element_type=F32)


def dot_nt(a_mat, b_mat):
    return lax.dot_general(a_mat, b_mat, (((1,), (1,)), ((), ())), preferred_element_type=F32)


def dot_tn(a_mat, b_mat):
    return lax.dot_general(a_mat, b_mat, (((0,), (0,)), ((), ())), preferred_element_type=F32)


class Place:
    def __init__(self, tokens, n_ffn):
        self.tokens, self.rows, self.n_ffn = tokens, tokens // 4, n_ffn
        self.hid = lax.axis_index("hid")
        self.ffn = lax.axis_index("ffn")
        self.chip, self.core = self.hid // 2, self.hid % 2
        self.core_peer = 2 * self.chip + (1 - self.core)
        self.chip_peer = 2 * (1 - self.chip) + self.core
        self.diag_peer = 2 * (1 - self.chip) + (1 - self.core)
        self.peers = []
        for dh in range(4):
            for df in range(n_ffn):
                if dh or df:
                    self.peers.append({"hid": (self.hid + dh) % 4, "ffn": (self.ffn + df) % n_ffn})

    def true_row(self, block):
        return self.rows * (2 * ((block // 2 + self.core) % 2) + (block % 2 + self.chip) % 2)

    def my_rows(self, ffn=None):
        return pl.ds(pl.multiple_of(self.rows * (self.ffn if ffn is None else ffn), self.rows), self.rows)

    def lanes(self):
        lane = lax.broadcasted_iota(jnp.int32, (self.tokens, LANES), 1)
        row = lax.broadcasted_iota(jnp.int32, (self.tokens, LANES), 0)
        rows = self.rows
        tok = rows * (2 * ((row // (2 * rows) + self.core) % 2) + ((row // rows) % 2 + self.chip) % 2) + row % rows
        return lane, tok

    def signal_all(self, barrier):
        for dev in self.peers:
            pl.semaphore_signal(barrier, inc=1, device_id=dev, device_id_type=MESH)


def rcopy(src, dst, ss, rs, dev):
    return pltpu.make_async_remote_copy(
        src_ref=src, dst_ref=dst, send_sem=ss, recv_sem=rs, device_id=dev, device_id_type=MESH)


def z_scatter(pos, part, sb, rb, ss, rs, sends):
    sb[...] = part[...].astype(BF)
    for df in range(1, pos.n_ffn):
        to = (pos.ffn + df) % pos.n_ffn
        c = rcopy(sb.at[pos.my_rows(to)], rb.at[df - 1], ss.at[df], rs.at[df], {"ffn": to})
        c.start()
        sends.append(c)


def z_total(pos, part, rb, ss, rs):
    tot = part[pos.my_rows(), :]
    for df in range(1, pos.n_ffn):
        rcopy(rb.at[df - 1], rb.at[df - 1], ss.at[df], rs.at[df], {"ffn": pos.ffn}).wait_recv()
        tot = tot + rb[df - 1].astype(F32)
    return tot


def z_gather(pos, buf, ss, rs, sends):
    mine = buf.at[pos.my_rows()]
    for df in range(1, pos.n_ffn):
        c = rcopy(mine, mine, ss.at[df], rs.at[pos.ffn], {"ffn": (pos.ffn + df) % pos.n_ffn})
        c.start()
        sends.append(c)


def z_gather_wait(pos, buf, ss, rs):
    for df in range(1, pos.n_ffn):
        frm = (pos.ffn + df) % pos.n_ffn
        blk = buf.at[pos.my_rows(frm)]
        rcopy(blk, blk, ss.at[df], rs.at[frm], {"ffn": frm}).wait_recv()


def stat_send(pos, st, ss, rs, ssq_v, c_v, sends):
    ln = lax.broadcasted_iota(jnp.int32, (pos.rows, LANES), 1)
    tid = pos.true_row(pos.ffn) + lax.broadcasted_iota(jnp.int32, (pos.rows, LANES), 0)
    val = jnp.where(ln == tid + pos.tokens, c_v, 0.0)
    if ssq_v is not None:
        val = val + jnp.where(ln == tid, ssq_v, 0.0)
    me = pos.hid * pos.n_ffn + pos.ffn
    st[me] = jnp.sum(val, axis=0, keepdims=True)
    for j, dev in enumerate(pos.peers):
        c = rcopy(st.at[me], st.at[me], ss.at[j], rs.at[me], dev)
        c.start()
        sends.append(c)


def stat_total(pos, st, ss, rs):
    for j, dev in enumerate(pos.peers):
        slot = dev["hid"] * pos.n_ffn + dev["ffn"]
        rcopy(st.at[slot], st.at[slot], ss.at[j], rs.at[slot], dev).wait_recv()
    tot = st[0]
    for s in range(1, 4 * pos.n_ffn):
        tot = tot + st[s]
    return tot


def step_kernel(
    dims,
    x_h, g1_h, g2_h, wg_h, wu_h, wd_h, wq_h, dxo_h, dq_h,
    wg, wu, wd, wq, dx_o, dg1_o, dg2_o, n1t, dgu,
    g1_ref, g2_ref, xv, ev, dxv, dqv, n1v, n2v, n2t, ebv, acc, own1, d2s, d2r, ys, yr, gu, av,
    own2, e2s, e2r, ys2, yr2, pq, dav,
    dn2r, zs, zr, x2v, zs2, zr2, dn1v, st1, st2, st3,
    ld_sem, w_sem,
    d2_ss, d2_rs, y_ss, y_rs, ag_ss, ag_rs, z_ss, z_rs, st_ss, st_rs,
):
    n_chunk, n_ffn, d_model = dims
    tokens, width = xv.shape
    rows = tokens // 4
    half = 2 * rows
    ffn_w = wg.shape[1]
    cw = ffn_w // n_chunk
    pos = Place(tokens, n_ffn)
    barrier = pltpu.get_barrier_semaphore()
    pos.signal_all(barrier)

    def load_rows(src, dst, slot):
        cps = []
        for j in range(4):
            r = pl.multiple_of(pos.true_row(j), rows)
            cps.append(pltpu.make_async_copy(
                src.at[pl.ds(r, rows), :], dst.at[pl.ds(rows * j, rows), :], ld_sem.at[slot + j]))
        return cps

    x_cp = load_rows(x_h, xv, 0)
    dq_cp = load_rows(dq_h, dqv, 4)
    dx_cp = load_rows(dxo_h, dxv, 8)
    wq_cp = pltpu.make_async_copy(wq_h, wq, ld_sem.at[12])
    g_cp = [pltpu.make_async_copy(g1_h, g1_ref, ld_sem.at[13]), pltpu.make_async_copy(g2_h, g2_ref, ld_sem.at[14])]
    for c in x_cp + g_cp:
        c.start()
    for c in dq_cp:
        c.start()
    wq_cp.start()
    w_cps, wd_cps = [], []
    for i in range(n_chunk):
        cols = pl.ds(i * cw, cw)
        w_cps.append([
            pltpu.make_async_copy(wg_h.at[:, cols], wg.at[:, cols], w_sem.at[0, i]),
            pltpu.make_async_copy(wu_h.at[:, cols], wu.at[:, cols], w_sem.at[1, i]),
        ])
        wd_cps.append(pltpu.make_async_copy(wd_h.at[cols, :], wd.at[cols, :], w_sem.at[2, i]))
    first = min(4, n_chunk)
    for i in range(first):
        for c in w_cps[i]:
            c.start()

    lane, tok_id = pos.lanes()
    for c in x_cp:
        c.wait()
    xf = xv[...].astype(F32)
    ssq = jnp.sum(xf * xf, axis=1, keepdims=True)
    st1[pos.hid] = jnp.sum(jnp.where(lane == tok_id, ssq, 0.0), axis=0, keepdims=True)
    pl.semaphore_wait(barrier, len(pos.peers))
    sends = []
    for k, dev in enumerate((pos.core_peer, pos.chip_peer, pos.diag_peer)):
        c = rcopy(st1.at[pos.hid], st1.at[pos.hid], st_ss.at[0, k], st_rs.at[0, pos.hid], {"hid": dev})
        c.start()
        sends.append(c)

    for c in dq_cp:
        c.wait()
    wq_cp.wait()
    for i in range(first, n_chunk):
        for c in w_cps[i]:
            c.start()
    for i in range(n_chunk):
        wd_cps[i].start()
    for c in dx_cp:
        c.start()
    qk = min(768, dqv.shape[1])
    acc[...] = dot_nt(dqv[:, :qk], wq[:, :qk])

    def dn2_body(k, _):
        cols = pl.ds(pl.multiple_of(k * qk, qk), qk)
        acc[...] += dot_nt(dqv[:, cols], wq[:, cols])
        return 0
    lax.fori_loop(1, dqv.shape[1] // qk, dn2_body, 0)
    dn2r[pos.ffn] = acc[...].astype(BF)
    for df in range(1, n_ffn):
        c = rcopy(dn2r.at[pos.ffn], dn2r.at[pos.ffn], z_ss.at[0, df], z_rs.at[0, pos.ffn],
                  {"ffn": (pos.ffn + df) % n_ffn})
        c.start()
        sends.append(c)

    for dev in (pos.core_peer, pos.chip_peer, pos.diag_peer):
        rcopy(st1.at[dev], st1.at[dev], st_ss.at[0, 0], st_rs.at[0, dev], {"hid": dev}).wait_recv()
    tot1 = (st1[0] + st1[1]) + (st1[2] + st1[3])
    mean1 = jnp.sum(jnp.where(lane == tok_id, tot1, 0.0), axis=1, keepdims=True) / d_model
    inv1 = lax.rsqrt(mean1 + NORM_EPS)
    for c in g_cp:
        c.wait()
    g1v = jnp.reshape(g1_ref[...], (1, width))
    g2v = jnp.reshape(g2_ref[...], (1, width))
    n1 = (xf * inv1 * g1v).astype(BF)
    n1v[...] = n1

    def fwd_a(i):
        for c in w_cps[i]:
            c.wait()
        for w_ref, base in ((wg, 0), (wu, cw)):
            p = dot_nn(n1v[...], w_ref[:, i * cw:(i + 1) * cw])
            own1[i, :, base:base + cw] = p[:half]
            d2s[i, :, base:base + cw] = p[half:]
        c = rcopy(d2s.at[i], d2r.at[i], d2_ss.at[0, i], d2_rs.at[0, i], {"hid": pos.core_peer})
        c.start()
        sends.append(c)

    def fwd_b(i):
        rcopy(d2s.at[i], d2r.at[i], d2_ss.at[0, i], d2_rs.at[0, i], {"hid": pos.core_peer}).wait_recv()
        ys[i] = (own1[i, rows:half] + d2r[i, rows:half]).astype(BF)
        c = rcopy(ys.at[i], yr.at[i], y_ss.at[0, i], y_rs.at[0, i], {"hid": pos.chip_peer})
        c.start()
        sends.append(c)
        gu[i] = own1[i, :rows] + d2r[i, :rows]

    def ag_chip(buf, ph, i):
        c = rcopy(buf.at[i, pl.ds(0, rows)], buf.at[i, pl.ds(rows, rows)],
                  ag_ss.at[ph, 0, i], ag_rs.at[ph, 0, i], {"hid": pos.chip_peer})
        c.start()
        sends.append(c)

    def ag_core(buf, ph, i):
        c = rcopy(buf.at[i, pl.ds(0, rows)], buf.at[i, pl.ds(half, rows)],
                  ag_ss.at[ph, 1, i], ag_rs.at[ph, 1, i], {"hid": pos.core_peer})
        c.start()
        sends.append(c)

    def ag_wait(buf, ph, lvl, i):
        blk = buf.at[i, pl.ds((lvl + 1) * rows, rows)]
        rcopy(blk, blk, ag_ss.at[ph, lvl, i], ag_rs.at[ph, lvl, i], {"hid": pos.core_peer}).wait_recv()

    def ag_forward(buf, ph, i):
        ag_wait(buf, ph, 0, i)
        c = rcopy(buf.at[i, pl.ds(rows, rows)], buf.at[i, pl.ds(3 * rows, rows)],
                  ag_ss.at[ph, 2, i], ag_rs.at[ph, 2, i], {"hid": pos.core_peer})
        c.start()
        sends.append(c)

    def fwd_c(i):
        rcopy(ys.at[i], yr.at[i], y_ss.at[0, i], y_rs.at[0, i], {"hid": pos.chip_peer}).wait_recv()
        tot = gu[i] + yr[i].astype(F32)
        g, u = tot[:, :cw], tot[:, cw:]
        sig = jax.nn.sigmoid(g)
        act = g * sig
        av[i, :rows] = (act * u).astype(BF)
        ag_chip(av, 0, i)
        ag_core(av, 0, i)
        pq[i, :rows, :cw] = (u * sig * (1.0 + g * (1.0 - sig))).astype(BF)
        pq[i, :rows, cw:] = act.astype(BF)

    def fwd_e(i):
        ag_wait(av, 0, 1, i)
        ag_wait(av, 0, 2, i)
        wd_cps[i].wait()
        p = dot_nn(av[i], wd[i * cw:(i + 1) * cw, :])
        if i == 0:
            acc[...] = p
        else:
            acc[...] += p

    def lagged(*stages):
        last = max(lag for _, lag in stages)
        for s in range(n_chunk + last):
            for fn, lag in stages:
                if 0 <= s - lag < n_chunk:
                    fn(s - lag)

    lagged((fwd_a, 0), (fwd_b, 1))
    n1t[...] = jnp.transpose(n1v[...])
    lagged((fwd_c, 0))
    ahead = (2 * n_chunk) // 3
    for i in range(ahead):
        ag_chip(pq, 1, i)
    lagged((lambda i: ag_forward(av, 0, i), 0), (fwd_e, 2))

    z_scatter(pos, acc, zs, zr, z_ss.at[1], z_rs.at[1], sends)
    for i in range(n_chunk):
        ag_core(pq, 1, i)
    for df in range(1, n_ffn):
        frm = (pos.ffn + df) % n_ffn
        rcopy(dn2r.at[frm], dn2r.at[frm], z_ss.at[0, df], z_rs.at[0, frm], {"ffn": frm}).wait_recv()
    dn2_tot = dn2r[0].astype(F32)
    for s in range(1, n_ffn):
        dn2_tot = dn2_tot + dn2r[s].astype(F32)
    ev[...] = dn2_tot
    my_rows = pos.my_rows()
    x2_rows = (xv[my_rows, :].astype(F32) + z_total(pos, acc, zr, z_ss.at[1], z_rs.at[1])).astype(BF)
    x2v[my_rows, :] = x2_rows
    z_gather(pos, x2v, z_ss.at[2], z_rs.at[2], sends)
    x2_f = x2_rows.astype(F32)
    stat_send(pos, st2, st_ss.at[1], st_rs.at[1],
              jnp.sum(x2_f * x2_f, axis=1, keepdims=True),
              jnp.sum(g2v * x2_f * ev[my_rows, :], axis=1, keepdims=True), sends)
    for i in range(ahead, n_chunk):
        ag_chip(pq, 1, i)
    for c in dx_cp:
        c.wait()
    z_gather_wait(pos, x2v, z_ss.at[2], z_rs.at[2])
    tot2 = stat_total(pos, st2, st_ss.at[1], st_rs.at[1])
    lane, tok_id = pos.lanes()
    inv2 = lax.rsqrt(jnp.sum(jnp.where(lane == tok_id, tot2, 0.0), axis=1, keepdims=True) / d_model + NORM_EPS)
    c2 = jnp.sum(jnp.where(lane == tok_id + tokens, tot2, 0.0), axis=1, keepdims=True)
    x2f = x2v[...].astype(F32)
    dn2 = ev[...]
    e_val = dxv[...].astype(F32) + (inv2 * (g2v * dn2) - x2f * (inv2 ** 3) * (c2 / d_model))
    ev[...] = e_val
    ebv[...] = e_val.astype(BF)
    n2v[...] = (x2f * inv2 * g2v).astype(BF)
    dg2_o[...] = jnp.sum(dn2 * x2f * inv2, axis=0)

    def bwd_a(i):
        p = dot_nt(ebv[...], wd[i * cw:(i + 1) * cw, :])
        own2[i] = p[:half]
        e2s[i] = p[half:]
        c = rcopy(e2s.at[i], e2r.at[i], d2_ss.at[1, i], d2_rs.at[1, i], {"hid": pos.core_peer})
        c.start()
        sends.append(c)

    def bwd_b(i):
        rcopy(e2s.at[i], e2r.at[i], d2_ss.at[1, i], d2_rs.at[1, i], {"hid": pos.core_peer}).wait_recv()
        ys2[i] = (own2[i, rows:half] + e2r[i, rows:half]).astype(BF)
        c = rcopy(ys2.at[i], yr2.at[i], y_ss.at[1, i], y_rs.at[1, i], {"hid": pos.chip_peer})
        c.start()
        sends.append(c)

    def bwd_c(i):
        rcopy(ys2.at[i], yr2.at[i], y_ss.at[1, i], y_rs.at[1, i], {"hid": pos.chip_peer}).wait_recv()
        d_act = own2[i, :rows] + e2r[i, :rows] + yr2[i].astype(F32)
        dav[i, :rows] = d_act.astype(BF)
        ag_chip(dav, 2, i)
        ag_core(dav, 2, i)

    def bwd_e(i):
        ag_wait(pq, 1, 1, i)
        ag_wait(pq, 1, 2, i)
        ag_wait(dav, 2, 1, i)
        ag_wait(dav, 2, 2, i)
        d_act = dav[i].astype(F32)
        dgu[i, :, :cw] = (d_act * pq[i, :, :cw].astype(F32)).astype(BF)
        dgu[i, :, cw:] = (d_act * pq[i, :, cw:].astype(F32)).astype(BF)
        cols = slice(i * cw, (i + 1) * cw)
        p = dot_nt(dgu[i, :, :cw], wg[:, cols]) + dot_nt(dgu[i, :, cw:], wu[:, cols])
        if i == 0:
            acc[...] = p
        else:
            acc[...] += p

    def fill_gate(i):
        cols = slice(i * cw, (i + 1) * cw)
        wg[:, cols] = dot_nn(n1t[...], dgu[i, :, :cw]).astype(BF)
        wu[:, cols] = dot_nn(n1t[...], dgu[i, :, cw:]).astype(BF)

    piece = min(256, cw)

    def fill_down(i):
        for t in range(cw // piece):
            r = i * cw + t * piece
            wd[r:r + piece, :] = dot_tn(av[i, :, t * piece:(t + 1) * piece], ebv[...]).astype(BF)

    qt = dqv.shape[1] // n_chunk

    def fill_qkv(i):
        cols = slice(i * qt, (i + 1) * qt)
        wq[:, cols] = dot_nn(n2t[...], dqv[:, cols]).astype(BF)

    lagged((bwd_a, 0), (bwd_b, 2))
    for i in range(n_chunk):
        ag_forward(pq, 1, i)
    n2t[...] = jnp.transpose(n2v[...])
    early = n_chunk // 3
    for i in range(early):
        fill_down(i)
    for i in range(n_chunk):
        bwd_c(i)
        if early + i < n_chunk:
            fill_down(early + i)
    lagged((lambda i: ag_forward(dav, 2, i), 0), (bwd_e, 1))

    z_scatter(pos, acc, zs2, zr2, z_ss.at[3], z_rs.at[3], sends)
    for i in range(n_chunk):
        fill_qkv(i)
    g1v = jnp.reshape(g1_ref[...], (1, width))
    dn1_rows = z_total(pos, acc, zr2, z_ss.at[3], z_rs.at[3]).astype(BF)
    dn1v[my_rows, :] = dn1_rows
    z_gather(pos, dn1v, z_ss.at[4], z_rs.at[4], sends)
    stat_send(pos, st3, st_ss.at[2], st_rs.at[2], None,
              jnp.sum(g1v * xv[my_rows, :].astype(F32) * dn1_rows.astype(F32), axis=1, keepdims=True), sends)
    for i in range(n_chunk - N_LATE):
        fill_gate(i)
    z_gather_wait(pos, dn1v, z_ss.at[4], z_rs.at[4])
    tot3 = stat_total(pos, st3, st_ss.at[2], st_rs.at[2])
    lane, tok_id = pos.lanes()
    c1 = jnp.sum(jnp.where(lane == tok_id + tokens, tot3, 0.0), axis=1, keepdims=True)
    tot1 = (st1[0] + st1[1]) + (st1[2] + st1[3])
    mean1 = jnp.sum(jnp.where(lane == tok_id, tot1, 0.0), axis=1, keepdims=True) / d_model
    inv1 = lax.rsqrt(mean1 + NORM_EPS)
    xf = xv[...].astype(F32)
    dn1 = dn1v[...].astype(F32)
    dx = (ev[...] + (inv1 * (g1v * dn1) - xf * (inv1 ** 3) * (c1 / d_model))).astype(BF)
    for j in range(4):
        dx_o[pl.ds(pl.multiple_of(pos.true_row(j), rows), rows), :] = dx[rows * j:rows * (j + 1)]
    dg1_o[...] = jnp.sum(dn1 * xf * inv1, axis=0)
    for c in sends:
        c.wait_send()


def store_kernel(*refs):
    n_part = 4
    srcs, n1t, dgu, dsts, sem, late_sem, late_buf = refs[:7], refs[7], refs[8], refs[9:16], refs[16], refs[17], refs[18]
    n_chunk, cw = dgu.shape[0], dgu.shape[2] // 2
    ready = (n_chunk - N_LATE) * cw
    cps = []
    for k in (2, 3, 0, 1):
        rows = srcs[k].shape[0] // n_part
        for j in range(n_part):
            idx = (pl.ds(j * rows, rows), pl.ds(0, ready)) if k < 2 else (pl.ds(j * rows, rows),)
            cps.append(pltpu.make_async_copy(srcs[k].at[idx], dsts[k].at[idx], sem.at[k, j]))
    for k in range(4, 7):
        cps.append(pltpu.make_async_copy(srcs[k], dsts[k], sem.at[k, 0]))
    for c in cps:
        c.start()
    for j in range(N_LATE):
        ch = n_chunk - N_LATE + j
        for k in range(2):
            late_buf[2 * j + k] = dot_nn(n1t[...], dgu[ch, :, k * cw:(k + 1) * cw]).astype(BF)
            c = pltpu.make_async_copy(late_buf.at[2 * j + k], dsts[k].at[:, pl.ds(ch * cw, cw)], late_sem.at[2 * j + k])
            c.start()
            cps.append(c)
    for c in cps:
        c.wait()


def solution(mesh):
    n_hid, n_ffn = mesh.shape["hid"], mesh.shape["ffn"]

    def local_step(x_in, gain_one, gain_two, w_gate, w_up, w_down, w_qkv, dx_out, d_qkv):
        tokens, width = x_in.shape
        ffn_w, qkv_w = w_gate.shape[1], w_qkv.shape[1]
        n_chunk = N_CHUNK
        cw = ffn_w // n_chunk
        rows = tokens // 4
        sds = jax.ShapeDtypeStruct
        vm = pltpu.VMEM
        dma = pltpu.SemaphoreType.DMA
        outs = pl.pallas_call(
            functools.partial(step_kernel, (n_chunk, n_ffn, width * n_hid)),
            out_shape=(
                vm((width, ffn_w), BF), vm((width, ffn_w), BF), vm((ffn_w, width), BF), vm((width, qkv_w), BF),
                vm((tokens, width), BF), vm((width,), F32), vm((width,), F32),
                vm((width, tokens), BF), vm((n_chunk, tokens, 2 * cw), BF),
            ),
            in_specs=[ANY] * 9,
            out_specs=(VM,) * 9,
            scratch_shapes=[
                vm((width,), F32), vm((width,), F32), vm((tokens, width), BF), vm((tokens, width), F32), vm((tokens, width), BF), vm((tokens, qkv_w), BF),
                vm((tokens, width), BF), vm((tokens, width), BF), vm((width, tokens), BF),
                vm((tokens, width), BF), vm((tokens, width), F32),
                vm((n_chunk, 2 * rows, 2 * cw), F32), vm((n_chunk, 2 * rows, 2 * cw), F32), vm((n_chunk, 2 * rows, 2 * cw), F32),
                vm((n_chunk, rows, 2 * cw), BF), vm((n_chunk, rows, 2 * cw), BF), vm((n_chunk, rows, 2 * cw), F32),
                vm((n_chunk, tokens, cw), BF),
                vm((n_chunk, 2 * rows, cw), F32), vm((n_chunk, 2 * rows, cw), F32), vm((n_chunk, 2 * rows, cw), F32),
                vm((n_chunk, rows, cw), BF), vm((n_chunk, rows, cw), BF),
                vm((n_chunk, tokens, 2 * cw), BF), vm((n_chunk, tokens, cw), BF),
                vm((n_ffn, tokens, width), BF),
                vm((tokens, width), BF), vm((n_ffn - 1, rows, width), BF), vm((tokens, width), BF),
                vm((tokens, width), BF), vm((n_ffn - 1, rows, width), BF), vm((tokens, width), BF),
                vm((4, 1, LANES), F32), vm((4 * n_ffn, 1, LANES), F32), vm((4 * n_ffn, 1, LANES), F32),
                dma((15,)), dma((3, n_chunk)),
                dma((2, n_chunk)), dma((2, n_chunk)), dma((2, n_chunk)), dma((2, n_chunk)),
                dma((3, 3, n_chunk)), dma((3, 3, n_chunk)), dma((5, n_ffn)), dma((5, n_ffn)),
                dma((3, 4 * n_ffn)), dma((3, 4 * n_ffn)),
            ],
            compiler_params=pltpu.CompilerParams(
                collective_id=0, has_side_effects=True, vmem_limit_bytes=30 * 2 ** 20),
            name="block_step",
        )(x_in, gain_one, gain_two, w_gate, w_up, w_down, w_qkv, dx_out, d_qkv)
        outs = [pltpu.with_memory_space_constraint(o, pltpu.VMEM) for o in outs]
        dw_gate, dw_up, dw_down, dw_qkv, dx_in, dg1, dg2 = pl.pallas_call(
            store_kernel,
            out_shape=tuple(sds(o.shape, o.dtype) for o in outs[:7]),
            in_specs=[VM] * 9,
            out_specs=(ANY,) * 7,
            scratch_shapes=[dma((7, 4)), dma((2 * N_LATE,)), vm((2 * N_LATE, width, cw), BF)],
            compiler_params=pltpu.CompilerParams(vmem_limit_bytes=30 * 2 ** 20),
            name="store_grads",
        )(*outs)
        return dx_in, dw_gate, dw_up, dw_down, dw_qkv, dg1, dg2

    tok_spec = P("data", "hid")
    in_specs = (tok_spec, P("hid"), P("hid"), P("hid", "ffn"), P("hid", "ffn"), P("ffn", "hid"), P("hid", "ffn"), tok_spec, P("data", "ffn"))
    out_specs = (tok_spec, P(("data", "hid"), "ffn"), P(("data", "hid"), "ffn"), P(("data", "ffn"), "hid"), P(("data", "hid"), "ffn"), P(("data", "hid")), P(("data", "hid")))
    return jax.shard_map(local_step, mesh=mesh, in_specs=in_specs, out_specs=out_specs, check_vma=False)
```

```python
import functools
import jax
import jax.numpy as jnp
from jax import lax
from jax.experimental import pallas as pl
from jax.experimental.pallas import tpu as pltpu
from jax.sharding import PartitionSpec as P

NORM_EPS = 1e-6
MESH = pl.DeviceIdType.MESH
ANY = pl.BlockSpec(memory_space=pl.ANY)
VM = pl.BlockSpec(memory_space=pltpu.VMEM)
BF = jnp.bfloat16
F32 = jnp.float32
LANES = 128
N_CHUNK = 6
N_LATE = 4


def dot_nn(a_mat, b_mat):
    return lax.dot_general(a_mat, b_mat, (((1,), (0,)), ((), ())), preferred_element_type=F32)


def dot_nt(a_mat, b_mat):
    return lax.dot_general(a_mat, b_mat, (((1,), (1,)), ((), ())), preferred_element_type=F32)


def dot_tn(a_mat, b_mat):
    return lax.dot_general(a_mat, b_mat, (((0,), (0,)), ((), ())), preferred_element_type=F32)


class Place:
    def __init__(self, tokens, n_ffn):
        self.tokens, self.rows, self.n_ffn = tokens, tokens // 4, n_ffn
        self.hid = lax.axis_index("hid")
        self.ffn = lax.axis_index("ffn")
        self.chip, self.core = self.hid // 2, self.hid % 2
        self.core_peer = 2 * self.chip + (1 - self.core)
        self.chip_peer = 2 * (1 - self.chip) + self.core
        self.diag_peer = 2 * (1 - self.chip) + (1 - self.core)
        self.dists = list(range(1, n_ffn))
        if n_ffn == 4:
            far, near = 3 - (self.ffn + 1) // 2, 1 + 2 * (self.ffn // 2)
            self.dists = [far, 6 - far - near, near]
        self.peers = []
        for dh in range(4):
            for df in range(n_ffn):
                if dh or df:
                    self.peers.append({"hid": (self.hid + dh) % 4, "ffn": (self.ffn + df) % n_ffn})

    def true_row(self, block):
        return self.rows * (2 * ((block // 2 + self.core) % 2) + (block % 2 + self.chip) % 2)

    def my_rows(self, ffn=None):
        return pl.ds(pl.multiple_of(self.rows * (self.ffn if ffn is None else ffn), self.rows), self.rows)

    def lanes(self):
        lane = lax.broadcasted_iota(jnp.int32, (self.tokens, LANES), 1)
        row = lax.broadcasted_iota(jnp.int32, (self.tokens, LANES), 0)
        rows = self.rows
        tok = rows * (2 * ((row // (2 * rows) + self.core) % 2) + ((row // rows) % 2 + self.chip) % 2) + row % rows
        return lane, tok

    def signal_near(self, barrier):
        near = [{"hid": h} for h in (self.core_peer, self.chip_peer, self.diag_peer)]
        near += [{"ffn": (self.ffn + df) % self.n_ffn} for df in range(1, self.n_ffn)]
        for dev in near:
            pl.semaphore_signal(barrier, inc=1, device_id=dev, device_id_type=MESH)
        return len(near)


def rcopy(src, dst, ss, rs, dev):
    return pltpu.make_async_remote_copy(
        src_ref=src, dst_ref=dst, send_sem=ss, recv_sem=rs, device_id=dev, device_id_type=MESH)


def z_scatter(pos, part, sb, rb, ss, rs, sends):
    sb[...] = part[...].astype(BF)
    for df in pos.dists:
        to = (pos.ffn + df) % pos.n_ffn
        c = rcopy(sb.at[pos.my_rows(to)], rb.at[df - 1], ss.at[df], rs.at[df], {"ffn": to})
        c.start()
        sends.append(c)


def z_total(pos, part, rb, ss, rs):
    tot = part[pos.my_rows(), :]
    for df in range(1, pos.n_ffn):
        rcopy(rb.at[df - 1], rb.at[df - 1], ss.at[df], rs.at[df], {"ffn": pos.ffn}).wait_recv()
        tot = tot + rb[df - 1].astype(F32)
    return tot


def z_gather(pos, buf, ss, rs, sends):
    mine = buf.at[pos.my_rows()]
    for df in pos.dists:
        c = rcopy(mine, mine, ss.at[df], rs.at[pos.ffn], {"ffn": (pos.ffn + df) % pos.n_ffn})
        c.start()
        sends.append(c)


def z_gather_wait(pos, buf, ss, rs):
    for df in range(1, pos.n_ffn):
        frm = (pos.ffn + df) % pos.n_ffn
        blk = buf.at[pos.my_rows(frm)]
        rcopy(blk, blk, ss.at[df], rs.at[frm], {"ffn": frm}).wait_recv()


def stat_send(pos, st, ss, rs, ssq_v, c_v, sends):
    ln = lax.broadcasted_iota(jnp.int32, (pos.rows, LANES), 1)
    tid = pos.true_row(pos.ffn) + lax.broadcasted_iota(jnp.int32, (pos.rows, LANES), 0)
    val = jnp.where(ln == tid + pos.tokens, c_v, 0.0)
    if ssq_v is not None:
        val = val + jnp.where(ln == tid, ssq_v, 0.0)
    me = pos.hid * pos.n_ffn + pos.ffn
    st[me] = jnp.sum(val, axis=0, keepdims=True)
    for j, dev in enumerate(pos.peers):
        c = rcopy(st.at[me], st.at[me], ss.at[j], rs.at[me], dev)
        c.start()
        sends.append(c)


def stat_total(pos, st, ss, rs):
    for j, dev in enumerate(pos.peers):
        slot = dev["hid"] * pos.n_ffn + dev["ffn"]
        rcopy(st.at[slot], st.at[slot], ss.at[j], rs.at[slot], dev).wait_recv()
    tot = st[0]
    for s in range(1, 4 * pos.n_ffn):
        tot = tot + st[s]
    return tot


def step_kernel(
    dims,
    x_h, g1_h, g2_h, wg_h, wu_h, wd_h, wq_h, dxo_h, dq_h,
    wg, wu, wd, wq, dx_o, dg1_o, dg2_o, n1t, dgu,
    g1_ref, g2_ref, xv, ev, dxv, dqv, n1v, n2v, n2t, ebv, acc, own1, d2s, d2r, ys, yr, gu, av,
    own2, e2s, e2r, ys2, yr2, pq, dav,
    dn2r, zs, zr, x2v, zs2, zr2, dn1v, st1, st2, st3,
    ld_sem, w_sem,
    d2_ss, d2_rs, y_ss, y_rs, ag_ss, ag_rs, z_ss, z_rs, st_ss, st_rs,
):
    n_chunk, n_ffn, d_model = dims
    tokens, width = xv.shape
    rows = tokens // 4
    half = 2 * rows
    ffn_w, qkv_w = wd.shape[0], dqv.shape[1]
    cw = ffn_w // n_chunk
    pos = Place(tokens, n_ffn)
    barrier = pltpu.get_barrier_semaphore()
    n_near = pos.signal_near(barrier)

    def load_rows(src, dst, slot):
        cps = []
        for j in range(4):
            r = pl.multiple_of(pos.true_row(j), rows)
            cps.append(pltpu.make_async_copy(
                src.at[pl.ds(r, rows), :], dst.at[pl.ds(rows * j, rows), :], ld_sem.at[slot + j]))
        return cps

    x_cp = load_rows(x_h, xv, 0)
    dq_cp = load_rows(dq_h, dqv, 4)
    dx_cp = load_rows(dxo_h, dxv, 8)
    wq_cp = pltpu.make_async_copy(wq_h, wq.at[:, pl.ds(0, qkv_w)], ld_sem.at[12])
    g_cp = [pltpu.make_async_copy(g1_h, g1_ref, ld_sem.at[13]), pltpu.make_async_copy(g2_h, g2_ref, ld_sem.at[14])]
    for c in x_cp + g_cp:
        c.start()
    for c in dq_cp:
        c.start()
    wq_cp.start()
    w_cps, wd_cps = [], []
    for i in range(n_chunk):
        cols = pl.ds(i * cw, cw)
        w_cps.append([
            pltpu.make_async_copy(wg_h.at[:, cols], wg.at[i, :, pl.ds(0, cw)], w_sem.at[0, i]),
            pltpu.make_async_copy(wu_h.at[:, cols], wu.at[i, :, pl.ds(0, cw)], w_sem.at[1, i]),
        ])
        wd_cps.append(pltpu.make_async_copy(wd_h.at[cols, :], wd.at[cols, :], w_sem.at[2, i]))
    first = min(4, n_chunk)
    for i in range(first):
        for c in w_cps[i]:
            c.start()

    lane, tok_id = pos.lanes()
    for c in x_cp:
        c.wait()
    xf = xv[...].astype(F32)
    ssq = jnp.sum(xf * xf, axis=1, keepdims=True)
    st1[pos.hid] = jnp.sum(jnp.where(lane == tok_id, ssq, 0.0), axis=0, keepdims=True)
    pl.semaphore_wait(barrier, n_near)
    sends = []
    for k, dev in enumerate((pos.core_peer, pos.chip_peer, pos.diag_peer)):
        c = rcopy(st1.at[pos.hid], st1.at[pos.hid], st_ss.at[0, k], st_rs.at[0, pos.hid], {"hid": dev})
        c.start()
        sends.append(c)

    for c in dq_cp:
        c.wait()
    wq_cp.wait()
    for i in range(first, n_chunk):
        for c in w_cps[i]:
            c.start()
    for i in range(n_chunk):
        wd_cps[i].start()
    for c in dx_cp:
        c.start()
    qk = min(768, dqv.shape[1])
    acc[...] = dot_nt(dqv[:, :qk], wq[:, :qk])

    def dn2_body(k, _):
        cols = pl.ds(pl.multiple_of(k * qk, qk), qk)
        acc[...] += dot_nt(dqv[:, cols], wq[:, cols])
        return 0
    lax.fori_loop(1, dqv.shape[1] // qk, dn2_body, 0)
    dn2r[pos.ffn] = acc[...].astype(BF)
    for df in range(1, n_ffn):
        c = rcopy(dn2r.at[pos.ffn], dn2r.at[pos.ffn], z_ss.at[0, df], z_rs.at[0, pos.ffn],
                  {"ffn": (pos.ffn + df) % n_ffn})
        c.start()
        sends.append(c)

    for dev in (pos.core_peer, pos.chip_peer, pos.diag_peer):
        rcopy(st1.at[dev], st1.at[dev], st_ss.at[0, 0], st_rs.at[0, dev], {"hid": dev}).wait_recv()
    tot1 = (st1[0] + st1[1]) + (st1[2] + st1[3])
    mean1 = jnp.sum(jnp.where(lane == tok_id, tot1, 0.0), axis=1, keepdims=True) / d_model
    inv1 = lax.rsqrt(mean1 + NORM_EPS)
    for c in g_cp:
        c.wait()
    g1v = jnp.reshape(g1_ref[...], (1, width))
    g2v = jnp.reshape(g2_ref[...], (1, width))
    n1 = (xf * inv1 * g1v).astype(BF)
    n1v[...] = n1

    def fwd_a(i):
        for c in w_cps[i]:
            c.wait()
        for w_ref, base in ((wg, 0), (wu, cw)):
            p = dot_nn(n1v[...], w_ref[i, :, :cw])
            own1[i, :, base:base + cw] = p[:half]
            d2s[i, :, base:base + cw] = p[half:]
        c = rcopy(d2s.at[i], d2r.at[i], d2_ss.at[0, i], d2_rs.at[0, i], {"hid": pos.core_peer})
        c.start()
        sends.append(c)

    def fwd_b(i):
        rcopy(d2s.at[i], d2r.at[i], d2_ss.at[0, i], d2_rs.at[0, i], {"hid": pos.core_peer}).wait_recv()
        ys[i] = (own1[i, rows:half] + d2r[i, rows:half]).astype(BF)
        c = rcopy(ys.at[i], yr.at[i], y_ss.at[0, i], y_rs.at[0, i], {"hid": pos.chip_peer})
        c.start()
        sends.append(c)
        gu[i] = own1[i, :rows] + d2r[i, :rows]

    def ag_chip(buf, ph, i):
        c = rcopy(buf.at[i, pl.ds(0, rows)], buf.at[i, pl.ds(rows, rows)],
                  ag_ss.at[ph, 0, i], ag_rs.at[ph, 0, i], {"hid": pos.chip_peer})
        c.start()
        sends.append(c)

    def ag_core(buf, ph, i):
        c = rcopy(buf.at[i, pl.ds(0, rows)], buf.at[i, pl.ds(half, rows)],
                  ag_ss.at[ph, 1, i], ag_rs.at[ph, 1, i], {"hid": pos.core_peer})
        c.start()
        sends.append(c)

    def ag_wait(buf, ph, lvl, i):
        blk = buf.at[i, pl.ds((lvl + 1) * rows, rows)]
        rcopy(blk, blk, ag_ss.at[ph, lvl, i], ag_rs.at[ph, lvl, i], {"hid": pos.core_peer}).wait_recv()

    def ag_forward(buf, ph, i):
        ag_wait(buf, ph, 0, i)
        c = rcopy(buf.at[i, pl.ds(rows, rows)], buf.at[i, pl.ds(3 * rows, rows)],
                  ag_ss.at[ph, 2, i], ag_rs.at[ph, 2, i], {"hid": pos.core_peer})
        c.start()
        sends.append(c)

    def fwd_c(i):
        rcopy(ys.at[i], yr.at[i], y_ss.at[0, i], y_rs.at[0, i], {"hid": pos.chip_peer}).wait_recv()
        tot = gu[i] + yr[i].astype(F32)
        g, u = tot[:, :cw], tot[:, cw:]
        sig = jax.nn.sigmoid(g)
        act = g * sig
        av[i, :rows] = (act * u).astype(BF)
        ag_chip(av, 0, i)
        ag_core(av, 0, i)
        pq[i, :rows, :cw] = (u * sig * (1.0 + g * (1.0 - sig))).astype(BF)
        pq[i, :rows, cw:] = act.astype(BF)

    def fwd_e(i):
        ag_wait(av, 0, 1, i)
        ag_wait(av, 0, 2, i)
        wd_cps[i].wait()
        p = dot_nn(av[i], wd[i * cw:(i + 1) * cw, :])
        if i == 0:
            acc[...] = p
        else:
            acc[...] += p

    def lagged(*stages):
        last = max(lag for _, lag in stages)
        for s in range(n_chunk + last):
            for fn, lag in stages:
                if 0 <= s - lag < n_chunk:
                    fn(s - lag)

    lagged((fwd_a, 0), (fwd_b, 1))
    n1t[...] = jnp.transpose(n1v[...])
    lagged((fwd_c, 0))
    ahead = (2 * n_chunk) // 3
    for i in range(ahead):
        ag_chip(pq, 1, i)
    lagged((lambda i: ag_forward(av, 0, i), 0), (fwd_e, 2))

    z_scatter(pos, acc, zs, zr, z_ss.at[1], z_rs.at[1], sends)
    for i in range(n_chunk):
        ag_core(pq, 1, i)
    for df in range(1, n_ffn):
        frm = (pos.ffn + df) % n_ffn
        rcopy(dn2r.at[frm], dn2r.at[frm], z_ss.at[0, df], z_rs.at[0, frm], {"ffn": frm}).wait_recv()
    dn2_tot = dn2r[0].astype(F32)
    for s in range(1, n_ffn):
        dn2_tot = dn2_tot + dn2r[s].astype(F32)
    ev[...] = dn2_tot
    my_rows = pos.my_rows()
    x2_rows = (xv[my_rows, :].astype(F32) + z_total(pos, acc, zr, z_ss.at[1], z_rs.at[1])).astype(BF)
    x2v[my_rows, :] = x2_rows
    z_gather(pos, x2v, z_ss.at[2], z_rs.at[2], sends)
    x2_f = x2_rows.astype(F32)
    stat_send(pos, st2, st_ss.at[1], st_rs.at[1],
              jnp.sum(x2_f * x2_f, axis=1, keepdims=True),
              jnp.sum(g2v * x2_f * ev[my_rows, :], axis=1, keepdims=True), sends)
    for i in range(ahead, n_chunk):
        ag_chip(pq, 1, i)
    for c in dx_cp:
        c.wait()
    z_gather_wait(pos, x2v, z_ss.at[2], z_rs.at[2])
    tot2 = stat_total(pos, st2, st_ss.at[1], st_rs.at[1])
    lane, tok_id = pos.lanes()
    inv2 = lax.rsqrt(jnp.sum(jnp.where(lane == tok_id, tot2, 0.0), axis=1, keepdims=True) / d_model + NORM_EPS)
    c2 = jnp.sum(jnp.where(lane == tok_id + tokens, tot2, 0.0), axis=1, keepdims=True)
    x2f = x2v[...].astype(F32)
    dn2 = ev[...]
    e_val = dxv[...].astype(F32) + (inv2 * (g2v * dn2) - x2f * (inv2 ** 3) * (c2 / d_model))
    ev[...] = e_val
    ebv[...] = e_val.astype(BF)
    n2v[...] = (x2f * inv2 * g2v).astype(BF)
    dg2_o[...] = jnp.sum(dn2 * x2f * inv2, axis=0)

    def bwd_a(i):
        p = dot_nt(ebv[...], wd[i * cw:(i + 1) * cw, :])
        own2[i] = p[:half]
        e2s[i] = p[half:]
        c = rcopy(e2s.at[i], e2r.at[i], d2_ss.at[1, i], d2_rs.at[1, i], {"hid": pos.core_peer})
        c.start()
        sends.append(c)

    def bwd_b(i):
        rcopy(e2s.at[i], e2r.at[i], d2_ss.at[1, i], d2_rs.at[1, i], {"hid": pos.core_peer}).wait_recv()
        ys2[i] = (own2[i, rows:half] + e2r[i, rows:half]).astype(BF)
        c = rcopy(ys2.at[i], yr2.at[i], y_ss.at[1, i], y_rs.at[1, i], {"hid": pos.chip_peer})
        c.start()
        sends.append(c)

    def bwd_c(i):
        rcopy(ys2.at[i], yr2.at[i], y_ss.at[1, i], y_rs.at[1, i], {"hid": pos.chip_peer}).wait_recv()
        d_act = own2[i, :rows] + e2r[i, :rows] + yr2[i].astype(F32)
        dav[i, :rows] = d_act.astype(BF)
        ag_chip(dav, 2, i)
        ag_core(dav, 2, i)

    def bwd_e(i):
        ag_wait(pq, 1, 1, i)
        ag_wait(pq, 1, 2, i)
        ag_wait(dav, 2, 1, i)
        ag_wait(dav, 2, 2, i)
        d_act = dav[i].astype(F32)
        dgu[i, :, :cw] = (d_act * pq[i, :, :cw].astype(F32)).astype(BF)
        dgu[i, :, cw:] = (d_act * pq[i, :, cw:].astype(F32)).astype(BF)
        p = dot_nt(dgu[i, :, :cw], wg[i, :, :cw]) + dot_nt(dgu[i, :, cw:], wu[i, :, :cw])
        if i == 0:
            acc[...] = p
        else:
            acc[...] += p

    def fill_gate(i):
        wg[i, :, :cw] = dot_nn(n1t[...], dgu[i, :, :cw]).astype(BF)
        wu[i, :, :cw] = dot_nn(n1t[...], dgu[i, :, cw:]).astype(BF)

    piece = min(256, cw)

    def fill_down(i):
        for t in range(cw // piece):
            r = i * cw + t * piece
            wd[r:r + piece, :] = dot_tn(av[i, :, t * piece:(t + 1) * piece], ebv[...]).astype(BF)

    qt = dqv.shape[1] // n_chunk

    def fill_qkv(i):
        cols = slice(i * qt, (i + 1) * qt)
        wq[:, cols] = dot_nn(n2t[...], dqv[:, cols]).astype(BF)

    lagged((bwd_a, 0), (bwd_b, 2))
    for i in range(n_chunk):
        ag_forward(pq, 1, i)
    n2t[...] = jnp.transpose(n2v[...])
    early = n_chunk // 3
    for i in range(early):
        fill_down(i)
    for i in range(n_chunk):
        bwd_c(i)
        if early + i < n_chunk:
            fill_down(early + i)
    lagged((lambda i: ag_forward(dav, 2, i), 0), (bwd_e, 1))

    z_scatter(pos, acc, zs2, zr2, z_ss.at[3], z_rs.at[3], sends)
    for i in range(n_chunk):
        fill_qkv(i)
    g1v = jnp.reshape(g1_ref[...], (1, width))
    dn1_rows = z_total(pos, acc, zr2, z_ss.at[3], z_rs.at[3]).astype(BF)
    dn1v[my_rows, :] = dn1_rows
    z_gather(pos, dn1v, z_ss.at[4], z_rs.at[4], sends)
    stat_send(pos, st3, st_ss.at[2], st_rs.at[2], None,
              jnp.sum(g1v * xv[my_rows, :].astype(F32) * dn1_rows.astype(F32), axis=1, keepdims=True), sends)
    for i in range(n_chunk - N_LATE):
        fill_gate(i)
    z_gather_wait(pos, dn1v, z_ss.at[4], z_rs.at[4])
    tot3 = stat_total(pos, st3, st_ss.at[2], st_rs.at[2])
    lane, tok_id = pos.lanes()
    c1 = jnp.sum(jnp.where(lane == tok_id + tokens, tot3, 0.0), axis=1, keepdims=True)
    tot1 = (st1[0] + st1[1]) + (st1[2] + st1[3])
    mean1 = jnp.sum(jnp.where(lane == tok_id, tot1, 0.0), axis=1, keepdims=True) / d_model
    inv1 = lax.rsqrt(mean1 + NORM_EPS)
    xf = xv[...].astype(F32)
    dn1 = dn1v[...].astype(F32)
    dx = (ev[...] + (inv1 * (g1v * dn1) - xf * (inv1 ** 3) * (c1 / d_model))).astype(BF)
    for j in range(4):
        dx_o[pl.ds(pl.multiple_of(pos.true_row(j), rows), rows), :] = dx[rows * j:rows * (j + 1)]
    dg1_o[...] = jnp.sum(dn1 * xf * inv1, axis=0)
    for c in sends:
        c.wait_send()


def store_kernel(*refs):
    n_part = 4
    srcs, n1t, dgu, dsts, sem, late_sem, late_buf = refs[:7], refs[7], refs[8], refs[9:16], refs[16], refs[17], refs[18]
    n_chunk, cw = dgu.shape[0], dgu.shape[2] // 2
    cps = []
    for k in (2, 3):
        rows, cols = dsts[k].shape[0] // n_part, dsts[k].shape[1]
        for j in range(n_part):
            part = pl.ds(j * rows, rows)
            cps.append(pltpu.make_async_copy(
                srcs[k].at[part, pl.ds(0, cols)], dsts[k].at[part, :], sem.at[k, j]))
    for k in range(2):
        for ch in range(n_chunk - N_LATE):
            cps.append(pltpu.make_async_copy(
                srcs[k].at[ch, :, pl.ds(0, cw)], dsts[k].at[:, pl.ds(ch * cw, cw)], sem.at[k, ch]))
    for k in range(4, 7):
        cps.append(pltpu.make_async_copy(srcs[k], dsts[k], sem.at[k, 0]))
    for c in cps:
        c.start()
    for j in range(N_LATE):
        ch = n_chunk - N_LATE + j
        for k in range(2):
            late_buf[2 * j + k, :, :cw] = dot_nn(n1t[...], dgu[ch, :, k * cw:(k + 1) * cw]).astype(BF)
            c = pltpu.make_async_copy(late_buf.at[2 * j + k, :, pl.ds(0, cw)], dsts[k].at[:, pl.ds(ch * cw, cw)], late_sem.at[2 * j + k])
            c.start()
            cps.append(c)
    for c in cps:
        c.wait()


def solution(mesh):
    n_hid, n_ffn = mesh.shape["hid"], mesh.shape["ffn"]

    def local_step(x_in, gain_one, gain_two, w_gate, w_up, w_down, w_qkv, dx_out, d_qkv):
        tokens, width = x_in.shape
        ffn_w, qkv_w = w_gate.shape[1], w_qkv.shape[1]
        n_chunk = N_CHUNK
        cw = ffn_w // n_chunk
        rows = tokens // 4
        sds = jax.ShapeDtypeStruct
        vm = pltpu.VMEM
        dma = pltpu.SemaphoreType.DMA
        outs = pl.pallas_call(
            functools.partial(step_kernel, (n_chunk, n_ffn, width * n_hid)),
            out_shape=(
                vm((n_chunk, width, cw + LANES), BF), vm((n_chunk, width, cw + LANES), BF), vm((ffn_w, width), BF), vm((width, qkv_w + LANES), BF),
                vm((tokens, width), BF), vm((width,), F32), vm((width,), F32),
                vm((width, tokens), BF), vm((n_chunk, tokens, 2 * cw), BF),
            ),
            in_specs=[ANY] * 9,
            out_specs=(VM,) * 9,
            scratch_shapes=[
                vm((width,), F32), vm((width,), F32), vm((tokens, width), BF), vm((tokens, width), F32), vm((tokens, width), BF), vm((tokens, qkv_w), BF),
                vm((tokens, width), BF), vm((tokens, width), BF), vm((width, tokens), BF),
                vm((tokens, width), BF), vm((tokens, width), F32),
                vm((n_chunk, 2 * rows, 2 * cw), F32), vm((n_chunk, 2 * rows, 2 * cw), F32), vm((n_chunk, 2 * rows, 2 * cw), F32),
                vm((n_chunk, rows, 2 * cw), BF), vm((n_chunk, rows, 2 * cw), BF), vm((n_chunk, rows, 2 * cw), F32),
                vm((n_chunk, tokens, cw), BF),
                vm((n_chunk, 2 * rows, cw), F32), vm((n_chunk, 2 * rows, cw), F32), vm((n_chunk, 2 * rows, cw), F32),
                vm((n_chunk, rows, cw), BF), vm((n_chunk, rows, cw), BF),
                vm((n_chunk, tokens, 2 * cw), BF), vm((n_chunk, tokens, cw), BF),
                vm((n_ffn, tokens, width), BF),
                vm((tokens, width), BF), vm((n_ffn - 1, rows, width), BF), vm((tokens, width), BF),
                vm((tokens, width), BF), vm((n_ffn - 1, rows, width), BF), vm((tokens, width), BF),
                vm((4, 1, LANES), F32), vm((4 * n_ffn, 1, LANES), F32), vm((4 * n_ffn, 1, LANES), F32),
                dma((15,)), dma((3, n_chunk)),
                dma((2, n_chunk)), dma((2, n_chunk)), dma((2, n_chunk)), dma((2, n_chunk)),
                dma((3, 3, n_chunk)), dma((3, 3, n_chunk)), dma((5, n_ffn)), dma((5, n_ffn)),
                dma((3, 4 * n_ffn)), dma((3, 4 * n_ffn)),
            ],
            compiler_params=pltpu.CompilerParams(
                collective_id=0, has_side_effects=True, vmem_limit_bytes=24 * 2 ** 20),
            name="block_step",
        )(x_in, gain_one, gain_two, w_gate, w_up, w_down, w_qkv, dx_out, d_qkv)
        outs = [pltpu.with_memory_space_constraint(o, pltpu.VMEM) for o in outs]
        dw_gate, dw_up, dw_down, dw_qkv, dx_in, dg1, dg2 = pl.pallas_call(
            store_kernel,
            out_shape=(
                sds((width, ffn_w), BF), sds((width, ffn_w), BF), sds((ffn_w, width), BF), sds((width, qkv_w), BF),
                sds((tokens, width), BF), sds((width,), F32), sds((width,), F32)),
            in_specs=[VM] * 9,
            out_specs=(ANY,) * 7,
            scratch_shapes=[dma((7, max(4, n_chunk))), dma((2 * N_LATE,)), vm((2 * N_LATE, width, cw + LANES), BF)],
            compiler_params=pltpu.CompilerParams(vmem_limit_bytes=24 * 2 ** 20),
            name="store_grads",
        )(*outs)
        return dx_in, dw_gate, dw_up, dw_down, dw_qkv, dg1, dg2

    tok_spec = P("data", "hid")
    in_specs = (tok_spec, P("hid"), P("hid"), P("hid", "ffn"), P("hid", "ffn"), P("ffn", "hid"), P("hid", "ffn"), tok_spec, P("data", "ffn"))
    out_specs = (tok_spec, P(("data", "hid"), "ffn"), P(("data", "hid"), "ffn"), P(("data", "ffn"), "hid"), P(("data", "hid"), "ffn"), P(("data", "hid")), P(("data", "hid")))
    return jax.shard_map(local_step, mesh=mesh, in_specs=in_specs, out_specs=out_specs, check_vma=False)
```

```python
import functools
import jax
import jax.numpy as jnp
from jax import lax
from jax.experimental import pallas as pl
from jax.experimental.pallas import tpu as pltpu
from jax.sharding import PartitionSpec as P

NORM_EPS = 1e-6
MESH = pl.DeviceIdType.MESH
ANY = pl.BlockSpec(memory_space=pl.ANY)
VM = pl.BlockSpec(memory_space=pltpu.VMEM)
BF = jnp.bfloat16
F32 = jnp.float32
LANES = 128
N_CHUNK = 6
N_LATE = 4


def dot_nn(a_mat, b_mat):
    return lax.dot_general(a_mat, b_mat, (((1,), (0,)), ((), ())), preferred_element_type=F32)


def dot_nt(a_mat, b_mat):
    return lax.dot_general(a_mat, b_mat, (((1,), (1,)), ((), ())), preferred_element_type=F32)


def dot_tn(a_mat, b_mat):
    return lax.dot_general(a_mat, b_mat, (((0,), (0,)), ((), ())), preferred_element_type=F32)


class Place:
    def __init__(self, tokens, n_ffn):
        self.tokens, self.rows, self.n_ffn = tokens, tokens // 4, n_ffn
        self.hid = lax.axis_index("hid")
        self.ffn = lax.axis_index("ffn")
        self.chip, self.core = self.hid // 2, self.hid % 2
        self.core_peer = 2 * self.chip + (1 - self.core)
        self.chip_peer = 2 * (1 - self.chip) + self.core
        self.diag_peer = 2 * (1 - self.chip) + (1 - self.core)
        self.dists = list(range(1, n_ffn))
        if n_ffn == 4:
            far, near = 3 - (self.ffn + 1) // 2, 1 + 2 * (self.ffn // 2)
            self.dists = [far, 6 - far - near, near]
        self.peers = []
        for df in self.dists + [0]:
            for dh in (2, 1, 3, 0):
                if dh or not isinstance(df, int) or df:
                    self.peers.append({"hid": (self.hid + dh) % 4, "ffn": (self.ffn + df) % n_ffn})

    def true_row(self, block):
        return self.rows * (2 * ((block // 2 + self.core) % 2) + (block % 2 + self.chip) % 2)

    def my_rows(self, ffn=None):
        return pl.ds(pl.multiple_of(self.rows * (self.ffn if ffn is None else ffn), self.rows), self.rows)

    def lanes(self):
        lane = lax.broadcasted_iota(jnp.int32, (self.tokens, LANES), 1)
        row = lax.broadcasted_iota(jnp.int32, (self.tokens, LANES), 0)
        rows = self.rows
        tok = rows * (2 * ((row // (2 * rows) + self.core) % 2) + ((row // rows) % 2 + self.chip) % 2) + row % rows
        return lane, tok

    def signal_near(self, barrier):
        near = [{"hid": h} for h in (self.core_peer, self.chip_peer, self.diag_peer)]
        near += [{"ffn": (self.ffn + df) % self.n_ffn} for df in range(1, self.n_ffn)]
        for dev in near:
            pl.semaphore_signal(barrier, inc=1, device_id=dev, device_id_type=MESH)
        return len(near)


def rcopy(src, dst, ss, rs, dev):
    return pltpu.make_async_remote_copy(
        src_ref=src, dst_ref=dst, send_sem=ss, recv_sem=rs, device_id=dev, device_id_type=MESH)


def z_scatter(pos, part, sb, rb, ss, rs, sends):
    sb[...] = part[...].astype(BF)
    for df in pos.dists:
        to = (pos.ffn + df) % pos.n_ffn
        c = rcopy(sb.at[pos.my_rows(to)], rb.at[df - 1], ss.at[df], rs.at[df], {"ffn": to})
        c.start()
        sends.append(c)


def z_total(pos, part, rb, ss, rs):
    tot = part[pos.my_rows(), :]
    for df in range(1, pos.n_ffn):
        rcopy(rb.at[df - 1], rb.at[df - 1], ss.at[df], rs.at[df], {"ffn": pos.ffn}).wait_recv()
        tot = tot + rb[df - 1].astype(F32)
    return tot


def z_gather(pos, buf, ss, rs, sends):
    mine = buf.at[pos.my_rows()]
    for df in pos.dists:
        c = rcopy(mine, mine, ss.at[df], rs.at[pos.ffn], {"ffn": (pos.ffn + df) % pos.n_ffn})
        c.start()
        sends.append(c)


def z_gather_wait(pos, buf, ss, rs):
    for df in range(1, pos.n_ffn):
        frm = (pos.ffn + df) % pos.n_ffn
        blk = buf.at[pos.my_rows(frm)]
        rcopy(blk, blk, ss.at[df], rs.at[frm], {"ffn": frm}).wait_recv()


def stat_send(pos, st, ss, rs, ssq_v, c_v, sends):
    ln = lax.broadcasted_iota(jnp.int32, (pos.rows, LANES), 1)
    tid = pos.true_row(pos.ffn) + lax.broadcasted_iota(jnp.int32, (pos.rows, LANES), 0)
    val = jnp.where(ln == tid + pos.tokens, c_v, 0.0)
    if ssq_v is not None:
        val = val + jnp.where(ln == tid, ssq_v, 0.0)
    me = pos.hid * pos.n_ffn + pos.ffn
    st[me] = jnp.sum(val, axis=0, keepdims=True)
    for j, dev in enumerate(pos.peers):
        c = rcopy(st.at[me], st.at[me], ss.at[j], rs.at[me], dev)
        c.start()
        sends.append(c)


def stat_total(pos, st, ss, rs):
    for j, dev in enumerate(pos.peers):
        slot = dev["hid"] * pos.n_ffn + dev["ffn"]
        rcopy(st.at[slot], st.at[slot], ss.at[j], rs.at[slot], dev).wait_recv()
    tot = st[0]
    for s in range(1, 4 * pos.n_ffn):
        tot = tot + st[s]
    return tot


def step_kernel(
    dims,
    x_h, g1_h, g2_h, wg_h, wu_h, wd_h, wq_h, dxo_h, dq_h,
    wg, wu, wd, wq, dx_o, dg1_o, dg2_o, n1t, dgu,
    g1_ref, g2_ref, xv, ev, dxv, dqv, n1v, n2v, n2t, ebv, acc, own1, d2s, d2r, ys, yr, gu, av,
    own2, e2s, e2r, ys2, yr2, pq, dav,
    dn2r, zs, zr, x2v, zs2, zr2, dn1v, st1, st2, st3,
    ld_sem, w_sem,
    d2_ss, d2_rs, y_ss, y_rs, ag_ss, ag_rs, z_ss, z_rs, st_ss, st_rs,
):
    n_chunk, n_ffn, d_model = dims
    tokens, width = xv.shape
    rows = tokens // 4
    half = 2 * rows
    ffn_w, qkv_w = wd.shape[0], dqv.shape[1]
    cw = ffn_w // n_chunk
    pos = Place(tokens, n_ffn)
    barrier = pltpu.get_barrier_semaphore()
    n_near = pos.signal_near(barrier)

    def load_rows(src, dst, slot):
        cps = []
        for j in range(4):
            r = pl.multiple_of(pos.true_row(j), rows)
            cps.append(pltpu.make_async_copy(
                src.at[pl.ds(r, rows), :], dst.at[pl.ds(rows * j, rows), :], ld_sem.at[slot + j]))
        return cps

    x_cp = load_rows(x_h, xv, 0)
    dq_cp = load_rows(dq_h, dqv, 4)
    dx_cp = load_rows(dxo_h, dxv, 8)
    wq_cp = pltpu.make_async_copy(wq_h, wq.at[:, pl.ds(0, qkv_w)], ld_sem.at[12])
    g_cp = [pltpu.make_async_copy(g1_h, g1_ref, ld_sem.at[13]), pltpu.make_async_copy(g2_h, g2_ref, ld_sem.at[14])]
    for c in x_cp + g_cp:
        c.start()
    for c in dq_cp:
        c.start()
    wq_cp.start()
    w_cps, wd_cps = [], []
    for i in range(n_chunk):
        cols = pl.ds(i * cw, cw)
        w_cps.append([
            pltpu.make_async_copy(wg_h.at[:, cols], wg.at[i, :, pl.ds(0, cw)], w_sem.at[0, i]),
            pltpu.make_async_copy(wu_h.at[:, cols], wu.at[i, :, pl.ds(0, cw)], w_sem.at[1, i]),
        ])
        wd_cps.append(pltpu.make_async_copy(wd_h.at[cols, :], wd.at[cols, :], w_sem.at[2, i]))
    first = min(1, n_chunk)
    for i in range(first):
        for c in w_cps[i]:
            c.start()

    lane, tok_id = pos.lanes()
    for c in x_cp:
        c.wait()
    xf = xv[...].astype(F32)
    ssq = jnp.sum(xf * xf, axis=1, keepdims=True)
    st1[pos.hid] = jnp.sum(jnp.where(lane == tok_id, ssq, 0.0), axis=0, keepdims=True)
    pl.semaphore_wait(barrier, n_near)
    sends = []
    for k, dev in enumerate((pos.core_peer, pos.chip_peer, pos.diag_peer)):
        c = rcopy(st1.at[pos.hid], st1.at[pos.hid], st_ss.at[0, k], st_rs.at[0, pos.hid], {"hid": dev})
        c.start()
        sends.append(c)

    for c in dq_cp:
        c.wait()
    wq_cp.wait()
    for i in range(first, min(3, n_chunk)):
        for c in w_cps[i]:
            c.start()
    qk = min(768, dqv.shape[1])
    acc[...] = dot_nt(dqv[:, :qk], wq[:, :qk])

    def dn2_body(k, _):
        cols = pl.ds(pl.multiple_of(k * qk, qk), qk)
        acc[...] += dot_nt(dqv[:, cols], wq[:, cols])
        return 0
    lax.fori_loop(1, dqv.shape[1] // qk, dn2_body, 0)
    dn2r[pos.ffn] = acc[...].astype(BF)
    for df in range(1, n_ffn):
        c = rcopy(dn2r.at[pos.ffn], dn2r.at[pos.ffn], z_ss.at[0, df], z_rs.at[0, pos.ffn],
                  {"ffn": (pos.ffn + df) % n_ffn})
        c.start()
        sends.append(c)

    for dev in (pos.core_peer, pos.chip_peer, pos.diag_peer):
        rcopy(st1.at[dev], st1.at[dev], st_ss.at[0, 0], st_rs.at[0, dev], {"hid": dev}).wait_recv()
    tot1 = (st1[0] + st1[1]) + (st1[2] + st1[3])
    mean1 = jnp.sum(jnp.where(lane == tok_id, tot1, 0.0), axis=1, keepdims=True) / d_model
    inv1 = lax.rsqrt(mean1 + NORM_EPS)
    for c in g_cp:
        c.wait()
    g1v = jnp.reshape(g1_ref[...], (1, width))
    g2v = jnp.reshape(g2_ref[...], (1, width))
    n1 = (xf * inv1 * g1v).astype(BF)
    n1v[...] = n1

    def fwd_a(i):
        for c in w_cps[i]:
            c.wait()
        if i + 3 < n_chunk:
            for c in w_cps[i + 3]:
                c.start()
        if i == n_chunk - 1:
            for c in wd_cps + dx_cp:
                c.start()
        for w_ref, base in ((wg, 0), (wu, cw)):
            p = dot_nn(n1v[...], w_ref[i, :, :cw])
            own1[i, :, base:base + cw] = p[:half]
            d2s[i, :, base:base + cw] = p[half:]
        c = rcopy(d2s.at[i], d2r.at[i], d2_ss.at[0, i], d2_rs.at[0, i], {"hid": pos.core_peer})
        c.start()
        sends.append(c)

    def fwd_b(i):
        rcopy(d2s.at[i], d2r.at[i], d2_ss.at[0, i], d2_rs.at[0, i], {"hid": pos.core_peer}).wait_recv()
        ys[i] = (own1[i, rows:half] + d2r[i, rows:half]).astype(BF)
        c = rcopy(ys.at[i], yr.at[i], y_ss.at[0, i], y_rs.at[0, i], {"hid": pos.chip_peer})
        c.start()
        sends.append(c)
        gu[i] = own1[i, :rows] + d2r[i, :rows]

    def ag_chip(buf, ph, i):
        c = rcopy(buf.at[i, pl.ds(0, rows)], buf.at[i, pl.ds(rows, rows)],
                  ag_ss.at[ph, 0, i], ag_rs.at[ph, 0, i], {"hid": pos.chip_peer})
        c.start()
        sends.append(c)

    def ag_core(buf, ph, i):
        c = rcopy(buf.at[i, pl.ds(0, rows)], buf.at[i, pl.ds(half, rows)],
                  ag_ss.at[ph, 1, i], ag_rs.at[ph, 1, i], {"hid": pos.core_peer})
        c.start()
        sends.append(c)

    def ag_wait(buf, ph, lvl, i):
        blk = buf.at[i, pl.ds((lvl + 1) * rows, rows)]
        rcopy(blk, blk, ag_ss.at[ph, lvl, i], ag_rs.at[ph, lvl, i], {"hid": pos.core_peer}).wait_recv()

    def ag_forward(buf, ph, i):
        ag_wait(buf, ph, 0, i)
        c = rcopy(buf.at[i, pl.ds(rows, rows)], buf.at[i, pl.ds(3 * rows, rows)],
                  ag_ss.at[ph, 2, i], ag_rs.at[ph, 2, i], {"hid": pos.core_peer})
        c.start()
        sends.append(c)

    def fwd_c(i):
        rcopy(ys.at[i], yr.at[i], y_ss.at[0, i], y_rs.at[0, i], {"hid": pos.chip_peer}).wait_recv()
        tot = gu[i] + yr[i].astype(F32)
        g, u = tot[:, :cw], tot[:, cw:]
        sig = jax.nn.sigmoid(g)
        act = g * sig
        av[i, :rows] = (act * u).astype(BF)
        ag_chip(av, 0, i)
        ag_core(av, 0, i)
        pq[i, :rows, :cw] = (u * sig * (1.0 + g * (1.0 - sig))).astype(BF)
        pq[i, :rows, cw:] = act.astype(BF)

    def fwd_e(i):
        ag_wait(av, 0, 1, i)
        ag_wait(av, 0, 2, i)
        wd_cps[i].wait()
        p = dot_nn(av[i], wd[i * cw:(i + 1) * cw, :])
        if i == 0:
            acc[...] = p
        else:
            acc[...] += p

    def lagged(*stages):
        last = max(lag for _, lag in stages)
        for s in range(n_chunk + last):
            for fn, lag in stages:
                if 0 <= s - lag < n_chunk:
                    fn(s - lag)

    lagged((fwd_a, 0), (fwd_b, 1))
    n1t[...] = jnp.transpose(n1v[...])
    lagged((fwd_c, 0))
    ahead = (2 * n_chunk) // 3
    for i in range(ahead):
        ag_chip(pq, 1, i)
    lagged((lambda i: ag_forward(av, 0, i), 0), (fwd_e, 2))

    z_scatter(pos, acc, zs, zr, z_ss.at[1], z_rs.at[1], sends)
    for i in range(n_chunk):
        ag_core(pq, 1, i)
    for df in range(1, n_ffn):
        frm = (pos.ffn + df) % n_ffn
        rcopy(dn2r.at[frm], dn2r.at[frm], z_ss.at[0, df], z_rs.at[0, frm], {"ffn": frm}).wait_recv()
    dn2_tot = dn2r[0].astype(F32)
    for s in range(1, n_ffn):
        dn2_tot = dn2_tot + dn2r[s].astype(F32)
    ev[...] = dn2_tot
    my_rows = pos.my_rows()
    x2_rows = (xv[my_rows, :].astype(F32) + z_total(pos, acc, zr, z_ss.at[1], z_rs.at[1])).astype(BF)
    x2v[my_rows, :] = x2_rows
    z_gather(pos, x2v, z_ss.at[2], z_rs.at[2], sends)
    x2_f = x2_rows.astype(F32)
    stat_send(pos, st2, st_ss.at[1], st_rs.at[1],
              jnp.sum(x2_f * x2_f, axis=1, keepdims=True),
              jnp.sum(g2v * x2_f * ev[my_rows, :], axis=1, keepdims=True), sends)
    for i in range(ahead, n_chunk):
        ag_chip(pq, 1, i)
    for c in dx_cp:
        c.wait()
    z_gather_wait(pos, x2v, z_ss.at[2], z_rs.at[2])
    tot2 = stat_total(pos, st2, st_ss.at[1], st_rs.at[1])
    lane, tok_id = pos.lanes()
    inv2 = lax.rsqrt(jnp.sum(jnp.where(lane == tok_id, tot2, 0.0), axis=1, keepdims=True) / d_model + NORM_EPS)
    c2 = jnp.sum(jnp.where(lane == tok_id + tokens, tot2, 0.0), axis=1, keepdims=True)
    x2f = x2v[...].astype(F32)
    dn2 = ev[...]
    e_val = dxv[...].astype(F32) + (inv2 * (g2v * dn2) - x2f * (inv2 ** 3) * (c2 / d_model))
    ev[...] = e_val
    ebv[...] = e_val.astype(BF)
    n2v[...] = (x2f * inv2 * g2v).astype(BF)
    dg2_o[...] = jnp.sum(dn2 * x2f * inv2, axis=0)

    def bwd_a(i):
        p = dot_nt(ebv[...], wd[i * cw:(i + 1) * cw, :])
        own2[i] = p[:half]
        e2s[i] = p[half:]
        c = rcopy(e2s.at[i], e2r.at[i], d2_ss.at[1, i], d2_rs.at[1, i], {"hid": pos.core_peer})
        c.start()
        sends.append(c)

    def bwd_b(i):
        rcopy(e2s.at[i], e2r.at[i], d2_ss.at[1, i], d2_rs.at[1, i], {"hid": pos.core_peer}).wait_recv()
        ys2[i] = (own2[i, rows:half] + e2r[i, rows:half]).astype(BF)
        c = rcopy(ys2.at[i], yr2.at[i], y_ss.at[1, i], y_rs.at[1, i], {"hid": pos.chip_peer})
        c.start()
        sends.append(c)

    def bwd_c(i):
        rcopy(ys2.at[i], yr2.at[i], y_ss.at[1, i], y_rs.at[1, i], {"hid": pos.chip_peer}).wait_recv()
        d_act = own2[i, :rows] + e2r[i, :rows] + yr2[i].astype(F32)
        dav[i, :rows] = d_act.astype(BF)
        ag_chip(dav, 2, i)
        ag_core(dav, 2, i)

    def bwd_e(i):
        ag_wait(pq, 1, 1, i)
        ag_wait(pq, 1, 2, i)
        ag_wait(dav, 2, 1, i)
        ag_wait(dav, 2, 2, i)
        d_act = dav[i].astype(F32)
        dgu[i, :, :cw] = (d_act * pq[i, :, :cw].astype(F32)).astype(BF)
        dgu[i, :, cw:] = (d_act * pq[i, :, cw:].astype(F32)).astype(BF)
        p = dot_nt(dgu[i, :, :cw], wg[i, :, :cw]) + dot_nt(dgu[i, :, cw:], wu[i, :, :cw])
        if i == 0:
            acc[...] = p
        else:
            acc[...] += p

    def fill_gate(i):
        wg[i, :, :cw] = dot_nn(n1t[...], dgu[i, :, :cw]).astype(BF)
        wu[i, :, :cw] = dot_nn(n1t[...], dgu[i, :, cw:]).astype(BF)

    piece = min(256, cw)

    def fill_down(i):
        for t in range(cw // piece):
            r = i * cw + t * piece
            wd[r:r + piece, :] = dot_tn(av[i, :, t * piece:(t + 1) * piece], ebv[...]).astype(BF)

    qt = dqv.shape[1] // n_chunk

    def fill_qkv(i):
        cols = slice(i * qt, (i + 1) * qt)
        wq[:, cols] = dot_nn(n2t[...], dqv[:, cols]).astype(BF)

    lagged((bwd_a, 0), (bwd_b, 2))
    for i in range(n_chunk):
        ag_forward(pq, 1, i)
    n2t[...] = jnp.transpose(n2v[...])
    early = n_chunk // 3
    for i in range(early):
        fill_down(i)
    for i in range(n_chunk):
        bwd_c(i)
        if early + i < n_chunk:
            fill_down(early + i)
    lagged((lambda i: ag_forward(dav, 2, i), 0), (bwd_e, 1))

    z_scatter(pos, acc, zs2, zr2, z_ss.at[3], z_rs.at[3], sends)
    for i in range(n_chunk):
        fill_qkv(i)
    g1v = jnp.reshape(g1_ref[...], (1, width))
    dn1_rows = z_total(pos, acc, zr2, z_ss.at[3], z_rs.at[3]).astype(BF)
    dn1v[my_rows, :] = dn1_rows
    z_gather(pos, dn1v, z_ss.at[4], z_rs.at[4], sends)
    stat_send(pos, st3, st_ss.at[2], st_rs.at[2], None,
              jnp.sum(g1v * xv[my_rows, :].astype(F32) * dn1_rows.astype(F32), axis=1, keepdims=True), sends)
    for i in range(n_chunk - N_LATE):
        fill_gate(i)
    z_gather_wait(pos, dn1v, z_ss.at[4], z_rs.at[4])
    tot3 = stat_total(pos, st3, st_ss.at[2], st_rs.at[2])
    lane, tok_id = pos.lanes()
    c1 = jnp.sum(jnp.where(lane == tok_id + tokens, tot3, 0.0), axis=1, keepdims=True)
    tot1 = (st1[0] + st1[1]) + (st1[2] + st1[3])
    mean1 = jnp.sum(jnp.where(lane == tok_id, tot1, 0.0), axis=1, keepdims=True) / d_model
    inv1 = lax.rsqrt(mean1 + NORM_EPS)
    xf = xv[...].astype(F32)
    dn1 = dn1v[...].astype(F32)
    dx = (ev[...] + (inv1 * (g1v * dn1) - xf * (inv1 ** 3) * (c1 / d_model))).astype(BF)
    for j in range(4):
        dx_o[pl.ds(pl.multiple_of(pos.true_row(j), rows), rows), :] = dx[rows * j:rows * (j + 1)]
    dg1_o[...] = jnp.sum(dn1 * xf * inv1, axis=0)
    for c in sends:
        c.wait_send()


def store_kernel(*refs):
    n_part = 4
    srcs, n1t, dgu, dsts, sem, late_sem, late_buf = refs[:7], refs[7], refs[8], refs[9:16], refs[16], refs[17], refs[18]
    n_chunk, cw = dgu.shape[0], dgu.shape[2] // 2
    cps = []
    for k in (2, 3):
        rows, cols = dsts[k].shape[0] // n_part, dsts[k].shape[1]
        for j in range(n_part):
            part = pl.ds(j * rows, rows)
            cps.append(pltpu.make_async_copy(
                srcs[k].at[part, pl.ds(0, cols)], dsts[k].at[part, :], sem.at[k, j]))
    for k in range(2):
        for ch in range(n_chunk - N_LATE):
            cps.append(pltpu.make_async_copy(
                srcs[k].at[ch, :, pl.ds(0, cw)], dsts[k].at[:, pl.ds(ch * cw, cw)], sem.at[k, ch]))
    for k in range(4, 7):
        cps.append(pltpu.make_async_copy(srcs[k], dsts[k], sem.at[k, 0]))
    for c in cps:
        c.start()
    for j in range(N_LATE):
        ch = n_chunk - N_LATE + j
        for k in range(2):
            late_buf[2 * j + k, :, :cw] = dot_nn(n1t[...], dgu[ch, :, k * cw:(k + 1) * cw]).astype(BF)
            c = pltpu.make_async_copy(late_buf.at[2 * j + k, :, pl.ds(0, cw)], dsts[k].at[:, pl.ds(ch * cw, cw)], late_sem.at[2 * j + k])
            c.start()
            cps.append(c)
    for c in cps:
        c.wait()


def solution(mesh):
    n_hid, n_ffn = mesh.shape["hid"], mesh.shape["ffn"]

    def local_step(x_in, gain_one, gain_two, w_gate, w_up, w_down, w_qkv, dx_out, d_qkv):
        tokens, width = x_in.shape
        ffn_w, qkv_w = w_gate.shape[1], w_qkv.shape[1]
        n_chunk = N_CHUNK
        cw = ffn_w // n_chunk
        rows = tokens // 4
        sds = jax.ShapeDtypeStruct
        vm = pltpu.VMEM
        dma = pltpu.SemaphoreType.DMA
        outs = pl.pallas_call(
            functools.partial(step_kernel, (n_chunk, n_ffn, width * n_hid)),
            out_shape=(
                vm((n_chunk, width, cw + LANES), BF), vm((n_chunk, width, cw + LANES), BF), vm((ffn_w, width), BF), vm((width, qkv_w + LANES), BF),
                vm((tokens, width), BF), vm((width,), F32), vm((width,), F32),
                vm((width, tokens), BF), vm((n_chunk, tokens, 2 * cw), BF),
            ),
            in_specs=[ANY] * 9,
            out_specs=(VM,) * 9,
            scratch_shapes=[
                vm((width,), F32), vm((width,), F32), vm((tokens, width), BF), vm((tokens, width), F32), vm((tokens, width), BF), vm((tokens, qkv_w), BF),
                vm((tokens, width), BF), vm((tokens, width), BF), vm((width, tokens), BF),
                vm((tokens, width), BF), vm((tokens, width), F32),
                vm((n_chunk, 2 * rows, 2 * cw), F32), vm((n_chunk, 2 * rows, 2 * cw), F32), vm((n_chunk, 2 * rows, 2 * cw), F32),
                vm((n_chunk, rows, 2 * cw), BF), vm((n_chunk, rows, 2 * cw), BF), vm((n_chunk, rows, 2 * cw), F32),
                vm((n_chunk, tokens, cw), BF),
                vm((n_chunk, 2 * rows, cw), F32), vm((n_chunk, 2 * rows, cw), F32), vm((n_chunk, 2 * rows, cw), F32),
                vm((n_chunk, rows, cw), BF), vm((n_chunk, rows, cw), BF),
                vm((n_chunk, tokens, 2 * cw), BF), vm((n_chunk, tokens, cw), BF),
                vm((n_ffn, tokens, width), BF),
                vm((tokens, width), BF), vm((n_ffn - 1, rows, width), BF), vm((tokens, width), BF),
                vm((tokens, width), BF), vm((n_ffn - 1, rows, width), BF), vm((tokens, width), BF),
                vm((4, 1, LANES), F32), vm((4 * n_ffn, 1, LANES), F32), vm((4 * n_ffn, 1, LANES), F32),
                dma((15,)), dma((3, n_chunk)),
                dma((2, n_chunk)), dma((2, n_chunk)), dma((2, n_chunk)), dma((2, n_chunk)),
                dma((3, 3, n_chunk)), dma((3, 3, n_chunk)), dma((5, n_ffn)), dma((5, n_ffn)),
                dma((3, 4 * n_ffn)), dma((3, 4 * n_ffn)),
            ],
            compiler_params=pltpu.CompilerParams(
                collective_id=0, has_side_effects=True, vmem_limit_bytes=24 * 2 ** 20),
            name="block_step",
        )(x_in, gain_one, gain_two, w_gate, w_up, w_down, w_qkv, dx_out, d_qkv)
        outs = [pltpu.with_memory_space_constraint(o, pltpu.VMEM) for o in outs]
        dw_gate, dw_up, dw_down, dw_qkv, dx_in, dg1, dg2 = pl.pallas_call(
            store_kernel,
            out_shape=(
                sds((width, ffn_w), BF), sds((width, ffn_w), BF), sds((ffn_w, width), BF), sds((width, qkv_w), BF),
                sds((tokens, width), BF), sds((width,), F32), sds((width,), F32)),
            in_specs=[VM] * 9,
            out_specs=(ANY,) * 7,
            scratch_shapes=[dma((7, max(4, n_chunk))), dma((2 * N_LATE,)), vm((2 * N_LATE, width, cw + LANES), BF)],
            compiler_params=pltpu.CompilerParams(vmem_limit_bytes=24 * 2 ** 20),
            name="store_grads",
        )(*outs)
        return dx_in, dw_gate, dw_up, dw_down, dw_qkv, dg1, dg2

    tok_spec = P("data", "hid")
    in_specs = (tok_spec, P("hid"), P("hid"), P("hid", "ffn"), P("hid", "ffn"), P("ffn", "hid"), P("hid", "ffn"), tok_spec, P("data", "ffn"))
    out_specs = (tok_spec, P(("data", "hid"), "ffn"), P(("data", "hid"), "ffn"), P(("data", "ffn"), "hid"), P(("data", "hid"), "ffn"), P(("data", "hid")), P(("data", "hid")))
    return jax.shard_map(local_step, mesh=mesh, in_specs=in_specs, out_specs=out_specs, check_vma=False)
```
